8 devices in a mesh: dp: 1 (over z), sp: 8 (over y, x, core).
Axes of the slice: x: 2, y: 2, z: 1, core: 2. Of those that a mesh axis runs over, the one named last changes fastest.
Arguments:
- hidden: bfloat16 [6144, 3072], P(('dp', 'sp'))
- positions: int32 [6144], P(('dp', 'sp'))
- d_attn: bfloat16 [6144, 3072], P(('dp', 'sp'))
- ln_weight: bfloat16 [3072], replicated
- w_q: bfloat16 [3072, 3072], replicated
- w_k: bfloat16 [3072, 1024], replicated
- w_v: bfloat16 [3072, 1024], replicated
- w_o: bfloat16 [3072, 3072], replicated
Outputs:
- output 1: bfloat16 [6144, 3072], P(('dp', 'sp'))
- output 2: bfloat16 [6144, 3072], P(('dp', 'sp'))
- output 3: bfloat16 [3072], P('dp')
- output 4: bfloat16 [3072, 3072], P('dp')
- output 5: bfloat16 [3072, 1024], P('dp')
- output 6: bfloat16 [3072, 1024], P('dp')
- output 7: bfloat16 [3072, 3072], P('dp')
All inputs are finite; a program needn't handle non-finite values.
Results may differ from the reference program's by a relative error of at most 0.0122927.
Values are sent between devices in bfloat16 or wider.
A program may use at most 1 GiB of HBM per device.

```python
import math
import jax
import jax.numpy as jnp
from jax import lax

MODEL_DIM = 3072
NUM_HEADS = 24
NUM_KV_HEADS = 8
HEAD_DIM = 128
SEQ_LEN = 6144
LN_EPS = 1e-5
ROPE_BASE = 10000.0
GROUP_SIZE = NUM_HEADS // NUM_KV_HEADS
ROW_BLOCK = math.gcd(SEQ_LEN, 64)
NUM_BLOCKS = SEQ_LEN // ROW_BLOCK
SCORE_SCALE = HEAD_DIM ** -0.5


def setup_inputs(seed: int = 0, part: int = 0) -> dict:
    base_key = jax.random.key(seed)
    part_keys = jax.random.split(jax.random.fold_in(base_key, part), 3)
    weight_keys = jax.random.split(base_key, 5)
    hidden = jax.random.normal(part_keys[0], (SEQ_LEN, MODEL_DIM), jnp.float32).astype(jnp.bfloat16)
    pos_steps = jax.random.randint(part_keys[1], (SEQ_LEN,), 1, 4, dtype=jnp.int32)
    positions = (jnp.cumsum(pos_steps) - pos_steps[0]).astype(jnp.int32)
    d_attn = jax.random.normal(part_keys[2], (SEQ_LEN, MODEL_DIM), jnp.float32).astype(jnp.bfloat16)
    ln_weight = (1.0 + 0.25 * jax.random.normal(weight_keys[0], (MODEL_DIM,), jnp.float32)).astype(jnp.bfloat16)
    q_scale = math.sqrt(math.log(SEQ_LEN) / MODEL_DIM)
    kv_scale = MODEL_DIM ** -0.5
    o_scale = (NUM_HEADS * HEAD_DIM) ** -0.5
    w_q = (jax.random.normal(weight_keys[1], (MODEL_DIM, NUM_HEADS * HEAD_DIM), jnp.float32) * q_scale).astype(jnp.bfloat16)
    w_k = (jax.random.normal(weight_keys[2], (MODEL_DIM, NUM_KV_HEADS * HEAD_DIM), jnp.float32) * kv_scale).astype(jnp.bfloat16)
    w_v = (jax.random.normal(weight_keys[3], (MODEL_DIM, NUM_KV_HEADS * HEAD_DIM), jnp.float32) * kv_scale).astype(jnp.bfloat16)
    w_o = (jax.random.normal(weight_keys[4], (NUM_HEADS * HEAD_DIM, MODEL_DIM), jnp.float32) * o_scale).astype(jnp.bfloat16)
    return {'hidden': hidden, 'positions': positions, 'd_attn': d_attn, 'ln_weight': ln_weight,
            'w_q': w_q, 'w_k': w_k, 'w_v': w_v, 'w_o': w_o}


def norm_f32(hid_f32, weight_f32):
    mean_val = jnp.mean(hid_f32, axis=-1, keepdims=True)
    centered = hid_f32 - mean_val
    var_val = jnp.mean(centered * centered, axis=-1, keepdims=True)
    return centered * lax.rsqrt(var_val + LN_EPS) * weight_f32


def rope_tables(positions):
    inv_freq = ROPE_BASE ** (-jnp.arange(0, HEAD_DIM, 2, dtype=jnp.float32) / HEAD_DIM)
    angles = positions.astype(jnp.float32)[:, None] * inv_freq[None, :]
    return jnp.cos(angles)[:, None, :], jnp.sin(angles)[:, None, :]


def apply_rope(values, cos_t, sin_t):
    rot_pairs = values.reshape(values.shape[:-1] + (HEAD_DIM // 2, 2))
    even_part = rot_pairs[..., 0]
    odd_part = rot_pairs[..., 1]
    new_even = even_part * cos_t - odd_part * sin_t
    new_odd = odd_part * cos_t + even_part * sin_t
    return jnp.stack([new_even, new_odd], axis=-1).reshape(values.shape)


def block_probs(q_f32, row_start, k_f32):
    scores = jnp.einsum('qgrd,kgd->grqk', q_f32, k_f32) * SCORE_SCALE
    row_ids = row_start + jnp.arange(ROW_BLOCK)
    col_ids = jnp.arange(SEQ_LEN)
    scores = jnp.where(row_ids[:, None] >= col_ids[None, :], scores, -jnp.inf)
    return jax.nn.softmax(scores, axis=-1)


def reference(hidden, positions, d_attn, ln_weight, w_q, w_k, w_v, w_o):
    normed32, norm_vjp = jax.vjp(norm_f32, hidden.astype(jnp.float32), ln_weight.astype(jnp.float32))
    normed = normed32.astype(jnp.bfloat16)
    cos_t, sin_t = rope_tables(positions)
    q_rot = apply_rope(jnp.dot(normed, w_q, preferred_element_type=jnp.float32).reshape(SEQ_LEN, NUM_HEADS, HEAD_DIM), cos_t, sin_t).astype(jnp.bfloat16)
    k_rot = apply_rope(jnp.dot(normed, w_k, preferred_element_type=jnp.float32).reshape(SEQ_LEN, NUM_KV_HEADS, HEAD_DIM), cos_t, sin_t).astype(jnp.bfloat16)
    v_all = jnp.dot(normed, w_v, preferred_element_type=jnp.float32).astype(jnp.bfloat16).reshape(SEQ_LEN, NUM_KV_HEADS, HEAD_DIM)
    q_grp = q_rot.reshape(NUM_BLOCKS, ROW_BLOCK, NUM_KV_HEADS, GROUP_SIZE, HEAD_DIM)
    k_f32 = k_rot.astype(jnp.float32)
    v_f32 = v_all.astype(jnp.float32)
    block_ids = jnp.arange(NUM_BLOCKS)

    def fwd_block(block_in):
        q_block, block_idx = block_in
        attn_prob = block_probs(q_block.astype(jnp.float32), block_idx * ROW_BLOCK, k_f32)
        prob_bf = attn_prob.astype(jnp.bfloat16).astype(jnp.float32)
        return jnp.einsum('grqk,kgd->qgrd', prob_bf, v_f32).astype(jnp.bfloat16)

    o_grp = lax.map(fwd_block, (q_grp, block_ids))
    o_tok = o_grp.reshape(SEQ_LEN, NUM_HEADS * HEAD_DIM)
    attn_out = jnp.dot(o_tok, w_o, preferred_element_type=jnp.float32).astype(jnp.bfloat16)
    d_o = jnp.dot(d_attn, w_o.T, preferred_element_type=jnp.float32).astype(jnp.bfloat16)
    dw_o = jnp.dot(o_tok.T, d_attn, preferred_element_type=jnp.float32)
    do_grp = d_o.reshape(NUM_BLOCKS, ROW_BLOCK, NUM_KV_HEADS, GROUP_SIZE, HEAD_DIM)

    def bwd_block(carry, block_in):
        dk_acc, dv_acc = carry
        q_block, do_block, block_idx = block_in
        q_f32 = q_block.astype(jnp.float32)
        do_f32 = do_block.astype(jnp.float32)
        attn_prob = block_probs(q_f32, block_idx * ROW_BLOCK, k_f32)
        prob_bf = attn_prob.astype(jnp.bfloat16).astype(jnp.float32)
        d_prob = jnp.einsum('qgrd,kgd->grqk', do_f32, v_f32)
        row_dot = jnp.sum(attn_prob * d_prob, axis=-1, keepdims=True)
        d_score = (attn_prob * (d_prob - row_dot) * SCORE_SCALE).astype(jnp.bfloat16).astype(jnp.float32)
        dq_block = jnp.einsum('grqk,kgd->qgrd', d_score, k_f32).astype(jnp.bfloat16)
        dk_acc = dk_acc + jnp.einsum('grqk,qgrd->kgd', d_score, q_f32)
        dv_acc = dv_acc + jnp.einsum('grqk,qgrd->kgd', prob_bf, do_f32)
        return (dk_acc, dv_acc), dq_block

    zero_acc = jnp.zeros((SEQ_LEN, NUM_KV_HEADS, HEAD_DIM), jnp.float32)
    kv_sums, dq_grp = lax.scan(bwd_block, (zero_acc, zero_acc), (q_grp, do_grp, block_ids))
    dk_bf = kv_sums[0].astype(jnp.bfloat16)
    dv_bf = kv_sums[1].astype(jnp.bfloat16)
    g_q = apply_rope(dq_grp.reshape(SEQ_LEN, NUM_HEADS, HEAD_DIM).astype(jnp.float32), cos_t, -sin_t).astype(jnp.bfloat16).reshape(SEQ_LEN, NUM_HEADS * HEAD_DIM)
    g_k = apply_rope(dk_bf.astype(jnp.float32), cos_t, -sin_t).astype(jnp.bfloat16).reshape(SEQ_LEN, NUM_KV_HEADS * HEAD_DIM)
    g_v = dv_bf.reshape(SEQ_LEN, NUM_KV_HEADS * HEAD_DIM)
    d_normed = (jnp.dot(g_q, w_q.T, preferred_element_type=jnp.float32)
                + jnp.dot(g_k, w_k.T, preferred_element_type=jnp.float32)
                + jnp.dot(g_v, w_v.T, preferred_element_type=jnp.float32))
    dw_q = jnp.dot(normed.T, g_q, preferred_element_type=jnp.float32)
    dw_k = jnp.dot(normed.T, g_k, preferred_element_type=jnp.float32)
    dw_v = jnp.dot(normed.T, g_v, preferred_element_type=jnp.float32)
    d_hid, d_lnw = norm_vjp(d_normed)
    return (attn_out, d_hid.astype(jnp.bfloat16), d_lnw.astype(jnp.bfloat16), dw_q.astype(jnp.bfloat16),
            dw_k.astype(jnp.bfloat16), dw_v.astype(jnp.bfloat16), dw_o.astype(jnp.bfloat16))
```

```python
import functools
import math
import jax
import jax.numpy as jnp
from jax import lax
from jax.experimental import pallas as pl
from jax.experimental.pallas import tpu as pltpu
from jax.sharding import PartitionSpec as P

D = 128
LN_EPS = 1e-5
ROPE_BASE = 10000.0
SCALE = D ** -0.5
SCALE2 = SCALE * math.log2(math.e)
NT = (((1,), (1,)), ((), ()))
f32 = jnp.float32
bf16 = jnp.bfloat16
VMEM_LIMIT = 60 * 2 ** 20


def rotate(val, cos, sin):
    even = lax.rem(lax.broadcasted_iota(jnp.int32, val.shape, 1), 2) == 0
    swapped = jnp.where(even, pltpu.roll(val, D - 1, 1), pltpu.roll(val, 1, 1))
    return val * cos + swapped * sin


def proj_kernel(h_ref, w_ref, cos_ref, sin_ref, q_ref, qt_ref, k_ref, v_ref, vt_ref, *, nh):
    h = h_ref[...]
    cos, sin = cos_ref[...], sin_ref[...]
    res = jnp.dot(h, w_ref[...], preferred_element_type=f32)
    for n in range(nh):
        rot = rotate(res[:, n * D:(n + 1) * D], cos, sin).astype(bf16)
        q_ref[:, n * D:(n + 1) * D] = rot
        qt_ref[n * D:(n + 1) * D, :] = rot.T
    k_ref[...] = rotate(res[:, nh * D:(nh + 1) * D], cos, sin).astype(bf16)
    v = res[:, (nh + 1) * D:].astype(bf16)
    v_ref[...] = v
    vt_ref[...] = v.T


def project(h, w, cos, sin, nh, bt=512):
    t, d = h.shape
    row = lambda c: pl.BlockSpec((bt, c), lambda i: (i, 0))
    col = lambda r: pl.BlockSpec((r, bt), lambda i: (0, i))
    return pl.pallas_call(
        functools.partial(proj_kernel, nh=nh),
        grid=(t // bt,),
        in_specs=[row(d), pl.BlockSpec((d, w.shape[1]), lambda i: (0, 0)), row(D), row(D)],
        out_specs=[row(nh * D), col(nh * D), row(D), row(D), col(D)],
        out_shape=[jax.ShapeDtypeStruct((t, nh * D), bf16), jax.ShapeDtypeStruct((nh * D, t), bf16),
                   jax.ShapeDtypeStruct((t, D), bf16), jax.ShapeDtypeStruct((t, D), bf16), jax.ShapeDtypeStruct((D, t), bf16)],
        compiler_params=pltpu.CompilerParams(vmem_limit_bytes=VMEM_LIMIT, dimension_semantics=("arbitrary",)),
        cost_estimate=pl.CostEstimate(flops=2 * t * d * w.shape[1], bytes_accessed=2 * t * d, transcendentals=0),
        name="qkv_proj")(h, w, cos, sin)


def dout_kernel(g_ref, w_ref, do_ref, dot_ref):
    val = lax.dot_general(g_ref[...], w_ref[...], NT, preferred_element_type=f32).astype(bf16)
    do_ref[...] = val
    dot_ref[...] = val.T


def dout_proj(g, w, bt=512):
    t, d = g.shape
    e = w.shape[0]
    return pl.pallas_call(
        dout_kernel,
        grid=(t // bt,),
        in_specs=[pl.BlockSpec((bt, d), lambda i: (i, 0)), pl.BlockSpec((e, d), lambda i: (0, 0))],
        out_specs=[pl.BlockSpec((bt, e), lambda i: (i, 0)), pl.BlockSpec((e, bt), lambda i: (0, i))],
        out_shape=[jax.ShapeDtypeStruct((t, e), bf16), jax.ShapeDtypeStruct((e, t), bf16)],
        compiler_params=pltpu.CompilerParams(vmem_limit_bytes=VMEM_LIMIT, dimension_semantics=("arbitrary",)),
        cost_estimate=pl.CostEstimate(flops=2 * t * d * e, bytes_accessed=2 * t * d, transcendentals=0),
        name="dout_proj")(g, w)


def fwd_kernel(q_ref, k_ref, vt_ref, o_ref, lse_ref, acc, ml, *, bq, bk, nh):
    i = pl.program_id(0)
    for h in range(nh):
        ml[2 * h:2 * h + 1, :] = jnp.full((1, bq), -1e30, f32)
        ml[2 * h + 1:2 * h + 2, :] = jnp.zeros((1, bq), f32)
    acc[...] = jnp.zeros_like(acc)

    def step(off, diag):
        kb = k_ref[pl.ds(off, bk), :]
        vt = vt_ref[:, pl.ds(off, bk)]
        if diag is not None:
            ki = lax.broadcasted_iota(jnp.int32, (bk, bq), 0) + diag
            qi = lax.broadcasted_iota(jnp.int32, (bk, bq), 1)
            keep = ki <= qi
        ss = [lax.dot_general(kb, q_ref[:, h * D:(h + 1) * D], NT, preferred_element_type=f32) for h in range(nh)]
        for h in range(nh):
            s = ss[h]
            if diag is not None:
                s = jnp.where(keep, s, -1e30)
            m_old = ml[2 * h:2 * h + 1, :]
            m_new = jnp.maximum(m_old, jnp.max(s, axis=0, keepdims=True))
            p = jnp.exp2(s * SCALE2 - m_new * SCALE2)
            alpha = jnp.exp2((m_old - m_new) * SCALE2)
            ml[2 * h:2 * h + 1, :] = m_new
            ml[2 * h + 1:2 * h + 2, :] = ml[2 * h + 1:2 * h + 2, :] * alpha + jnp.sum(p, axis=0, keepdims=True)
            pv = jnp.dot(vt, p.astype(bf16), preferred_element_type=f32)
            acc[h * D:(h + 1) * D, :] = acc[h * D:(h + 1) * D, :] * alpha + pv

    ratio = bq // bk

    def body(j, carry):
        step(pl.multiple_of(j * bk, bk), None)
        return carry

    lax.fori_loop(0, i * ratio, body, 0)
    for d in range(ratio):
        step(pl.multiple_of(i * bq + d * bk, bk), d * bk)
    for h in range(nh):
        m = ml[2 * h:2 * h + 1, :]
        l = ml[2 * h + 1:2 * h + 2, :]
        out_t = acc[h * D:(h + 1) * D, :] * (1.0 / l)
        o_ref[:, h * D:(h + 1) * D] = out_t.T.astype(bf16)
        lse_ref[:, h * D:(h + 1) * D] = jnp.broadcast_to(m * SCALE2 + jnp.log2(l), (D, bq)).T


def attn_fwd(q, k, vt, bq=1024, bk=512):
    t, e = q.shape
    nh = e // D
    row = pl.BlockSpec((bq, e), lambda i: (i, 0))
    return pl.pallas_call(
        functools.partial(fwd_kernel, bq=bq, bk=bk, nh=nh),
        grid=(t // bq,),
        in_specs=[row, pl.BlockSpec((t, D), lambda i: (0, 0)), pl.BlockSpec((D, t), lambda i: (0, 0))],
        out_specs=[row, row],
        out_shape=[jax.ShapeDtypeStruct((t, e), bf16), jax.ShapeDtypeStruct((t, e), f32)],
        scratch_shapes=[pltpu.VMEM((e, bq), f32), pltpu.VMEM((8, bq), f32)],
        compiler_params=pltpu.CompilerParams(vmem_limit_bytes=VMEM_LIMIT, dimension_semantics=("arbitrary",)),
        cost_estimate=pl.CostEstimate(flops=4 * t * t * e, bytes_accessed=8 * t * e, transcendentals=0),
        name="attn_fwd")(q, k, vt)


def bwd_kernel(q_ref, qt_ref, do_ref, dot_ref, o_ref, lse_ref, k_ref, v_ref, cos_ref, sin_ref,
               dq_ref, dk_ref, dv_ref, dlt, dqa, dka, dva, *, bq, bk, t, nh):
    h = pl.program_id(0)
    j = pl.program_id(1)
    nq = t // bq
    rep = bk // D
    koff = pl.multiple_of(j * bk, bk)
    kc = pl.ds(koff, bk)

    @pl.when(j == 0)
    def _():
        def init(i, carry):
            r = pl.ds(pl.multiple_of(i * bq, bq), bq)
            d = jnp.sum(do_ref[r, :].astype(f32) * o_ref[r, :].astype(f32), axis=1, keepdims=True)
            dlt[r, :] = jnp.broadcast_to(d, (bq, D))
            dqa[r, :] = jnp.zeros((bq, D), f32)
            return carry
        lax.fori_loop(0, nq, init, 0)

    @pl.when(h == 0)
    def _():
        dka[:, kc] = jnp.zeros((D, bk), f32)
        dva[:, kc] = jnp.zeros((D, bk), f32)

    kb = k_ref[...]
    vb = v_ref[...]

    def step(i, diag):
        off = pl.multiple_of(i * bq, bq)
        r = pl.ds(off, bq)
        s = lax.dot_general(q_ref[r, :], kb, NT, preferred_element_type=f32)
        dp = lax.dot_general(do_ref[r, :], vb, NT, preferred_element_type=f32)
        if diag:
            qi = lax.broadcasted_iota(jnp.int32, (bq, bk), 0) + (off - koff)
            ki = lax.broadcasted_iota(jnp.int32, (bq, bk), 1)
            s = jnp.where(ki <= qi, s, -1e30)
        p = jnp.exp2(s * SCALE2 - jnp.concatenate([lse_ref[r, :]] * rep, axis=1))
        ds = ((dp - jnp.concatenate([dlt[r, :]] * rep, axis=1)) * p * SCALE).astype(bf16)
        dva[:, kc] += jnp.dot(dot_ref[:, r], p.astype(bf16), preferred_element_type=f32)
        dka[:, kc] += jnp.dot(qt_ref[:, r], ds, preferred_element_type=f32)
        dqa[r, :] += jnp.dot(ds, kb, preferred_element_type=f32)

    ratio = max(bk // bq, 1)
    first = (j * bk) // bq
    for d in range(ratio):
        step(first + d, True)

    def body(i, carry):
        step(i, False)
        return carry

    lax.fori_loop(first + ratio, nq, body, 0)

    @pl.when(j == pl.num_programs(1) - 1)
    def _():
        def fin(i, carry):
            r = pl.ds(pl.multiple_of(i * bq, bq), bq)
            dq = dqa[r, :].astype(bf16).astype(f32)
            dq_ref[r, :] = rotate(dq, cos_ref[r, :], -sin_ref[r, :]).astype(bf16)
            return carry
        lax.fori_loop(0, nq, fin, 0)

    @pl.when(h == nh - 1)
    def _():
        dk = dka[:, kc].T.astype(bf16).astype(f32)
        dk_ref[...] = rotate(dk, cos_ref[kc, :], -sin_ref[kc, :]).astype(bf16)
        dv_ref[...] = dva[:, kc].T.astype(bf16)


def attn_bwd(q, qt, do, dot, o, lse, k, v, cos, sin, bq=512, bk=1024):
    t, e = q.shape
    nh = e // D
    col = pl.BlockSpec((t, D), lambda h, j: (0, h))
    row_t = pl.BlockSpec((D, t), lambda h, j: (h, 0))
    kv_in = pl.BlockSpec((bk, D), lambda h, j: (j, 0))
    kv_out = pl.BlockSpec((bk, D), lambda h, j: (jnp.where(h == nh - 1, j, 0), 0))
    table = pl.BlockSpec((t, D), lambda h, j: (0, 0), pipeline_mode=pl.Buffered(1))
    return pl.pallas_call(
        functools.partial(bwd_kernel, bq=bq, bk=bk, t=t, nh=nh),
        grid=(nh, t // bk),
        in_specs=[col, row_t, col, row_t, col, col, kv_in, kv_in, table, table],
        out_specs=[col, kv_out, kv_out],
        out_shape=[jax.ShapeDtypeStruct((t, e), bf16), jax.ShapeDtypeStruct((t, D), bf16), jax.ShapeDtypeStruct((t, D), bf16)],
        scratch_shapes=[pltpu.VMEM((t, D), f32), pltpu.VMEM((t, D), f32), pltpu.VMEM((D, t), f32), pltpu.VMEM((D, t), f32)],
        compiler_params=pltpu.CompilerParams(vmem_limit_bytes=VMEM_LIMIT, dimension_semantics=("arbitrary", "arbitrary")),
        cost_estimate=pl.CostEstimate(flops=10 * t * t * e, bytes_accessed=20 * t * e, transcendentals=0),
        name="attn_bwd")(q, qt, do, dot, o, lse, k, v, cos, sin)


def norm_f32(hid_f32, weight_f32):
    mean_val = jnp.mean(hid_f32, axis=-1, keepdims=True)
    centered = hid_f32 - mean_val
    var_val = jnp.mean(centered * centered, axis=-1, keepdims=True)
    return centered * lax.rsqrt(var_val + LN_EPS) * weight_f32


def rope_tables(positions):
    lane = jnp.arange(D, dtype=jnp.int32)
    inv_freq = ROPE_BASE ** (-(lane - lane % 2).astype(f32) / D)
    angles = positions.astype(f32)[:, None] * inv_freq[None, :]
    sin = jnp.sin(angles)
    return jnp.cos(angles), jnp.where(lane[None, :] % 2 == 0, -sin, sin)


def solution(mesh):
    n_dev = mesh.shape['sp']
    row_spec = P(('dp', 'sp'), None)
    pos_spec = P(('dp', 'sp'))
    full_spec = P(None, None)
    grad_spec = P('dp', None)

    def local_step(hidden, positions, d_attn, ln_weight, w_q, w_k, w_v, w_o):
        rows, dim = hidden.shape
        idx = lax.axis_index('sp')
        qe = w_q.shape[1] // n_dev
        ke = w_k.shape[1] // n_dev
        normed32, norm_vjp = jax.vjp(norm_f32, hidden.astype(f32), ln_weight.astype(f32))
        h_all = lax.all_gather(normed32.astype(bf16), 'sp', axis=0, tiled=True)
        g_all = lax.all_gather(d_attn, 'sp', axis=0, tiled=True)
        cos, sin = rope_tables(lax.all_gather(positions, 'sp', axis=0, tiled=True))
        w_own = jnp.concatenate([lax.dynamic_slice_in_dim(w_q, idx * qe, qe, 1), lax.dynamic_slice_in_dim(w_k, idx * ke, ke, 1),
                                 lax.dynamic_slice_in_dim(w_v, idx * ke, ke, 1)], axis=1)
        wo_own = lax.dynamic_slice_in_dim(w_o, idx * qe, qe, 0)
        q, qt, k, v, vt = project(h_all, w_own, cos, sin, qe // D)
        o, lse = attn_fwd(q, k, vt)
        o_tok = lax.all_to_all(o.reshape(n_dev, rows, qe), 'sp', 0, 0)
        attn_out = jnp.einsum('stn,snd->td', o_tok, w_o.reshape(n_dev, qe, dim), preferred_element_type=f32).astype(bf16)
        do, dot = dout_proj(g_all, wo_own)
        dwo_own = jnp.einsum('te,td->ed', o, g_all, preferred_element_type=f32).astype(bf16)
        dw_o = lax.all_gather(dwo_own, 'sp', axis=0, tiled=True)
        gq, gk, gv = attn_bwd(q, qt, do, dot, o, lse, k, v, cos, sin)
        g_own = jnp.concatenate([gq, gk, gv], axis=1)
        g_tok = lax.all_to_all(g_own.reshape(n_dev, rows, qe + 2 * ke), 'sp', 0, 0)
        dw_own = jnp.einsum('te,td->ed', g_own, h_all, preferred_element_type=f32).astype(bf16)
        dw_all = lax.all_gather(dw_own, 'sp', axis=0, tiled=False)
        dw_q = dw_all[:, :qe].reshape(n_dev * qe, dim).T
        dw_k = dw_all[:, qe:qe + ke].reshape(n_dev * ke, dim).T
        dw_v = dw_all[:, qe + ke:].reshape(n_dev * ke, dim).T
        d_normed = (jnp.einsum('ste,dse->td', g_tok[:, :, :qe], w_q.reshape(dim, n_dev, qe), preferred_element_type=f32)
                    + jnp.einsum('ste,dse->td', g_tok[:, :, qe:qe + ke], w_k.reshape(dim, n_dev, ke), preferred_element_type=f32)
                    + jnp.einsum('ste,dse->td', g_tok[:, :, qe + ke:], w_v.reshape(dim, n_dev, ke), preferred_element_type=f32))
        d_hid, d_lnw = norm_vjp(d_normed)
        return (attn_out, d_hid.astype(bf16), lax.psum(d_lnw, 'sp').astype(bf16), dw_q, dw_k, dw_v, dw_o)

    return jax.shard_map(local_step, mesh=mesh,
                         in_specs=(row_spec, pos_spec, row_spec, P(None), full_spec, full_spec, full_spec, full_spec),
                         out_specs=(row_spec, row_spec, P('dp'), grad_spec, grad_spec, grad_spec, grad_spec),
                         check_vma=False)
```

```python
import functools
import math
import jax
import jax.numpy as jnp
from jax import lax
from jax.experimental import pallas as pl
from jax.experimental.pallas import tpu as pltpu
from jax.sharding import PartitionSpec as P

D = 128
LN_EPS = 1e-5
ROPE_BASE = 10000.0
SCALE = D ** -0.5
SCALE2 = SCALE * math.log2(math.e)
NT = (((1,), (1,)), ((), ()))
f32 = jnp.float32
bf16 = jnp.bfloat16
VMEM_LIMIT = 60 * 2 ** 20


def rotate(val, cos, sin):
    even = lax.rem(lax.broadcasted_iota(jnp.int32, val.shape, 1), 2) == 0
    swapped = jnp.where(even, pltpu.roll(val, D - 1, 1), pltpu.roll(val, 1, 1))
    return val * cos + swapped * sin


def proj_kernel(h_ref, w_ref, cos_ref, sin_ref, q_ref, qt_ref, k_ref, v_ref, vt_ref, *, nh):
    h = h_ref[...]
    cos, sin = cos_ref[...], sin_ref[...]
    res = jnp.dot(h, w_ref[...], preferred_element_type=f32)
    for n in range(nh):
        rot = rotate(res[:, n * D:(n + 1) * D], cos, sin).astype(bf16)
        q_ref[:, n * D:(n + 1) * D] = rot
        qt_ref[n * D:(n + 1) * D, :] = rot.T
    k_ref[...] = rotate(res[:, nh * D:(nh + 1) * D], cos, sin).astype(bf16)
    v = res[:, (nh + 1) * D:].astype(bf16)
    v_ref[...] = v
    vt_ref[...] = v.T


def project(h, w, cos, sin, nh, bt=512):
    t, d = h.shape
    row = lambda c: pl.BlockSpec((bt, c), lambda i: (i, 0))
    col = lambda r: pl.BlockSpec((r, bt), lambda i: (0, i))
    return pl.pallas_call(
        functools.partial(proj_kernel, nh=nh),
        grid=(t // bt,),
        in_specs=[row(d), pl.BlockSpec((d, w.shape[1]), lambda i: (0, 0)), row(D), row(D)],
        out_specs=[row(nh * D), col(nh * D), row(D), row(D), col(D)],
        out_shape=[jax.ShapeDtypeStruct((t, nh * D), bf16), jax.ShapeDtypeStruct((nh * D, t), bf16),
                   jax.ShapeDtypeStruct((t, D), bf16), jax.ShapeDtypeStruct((t, D), bf16), jax.ShapeDtypeStruct((D, t), bf16)],
        compiler_params=pltpu.CompilerParams(vmem_limit_bytes=VMEM_LIMIT, dimension_semantics=("arbitrary",)),
        cost_estimate=pl.CostEstimate(flops=2 * t * d * w.shape[1], bytes_accessed=2 * t * d, transcendentals=0),
        name="qkv_proj")(h, w, cos, sin)


def dout_kernel(g_ref, w_ref, do_ref, dot_ref):
    val = lax.dot_general(g_ref[...], w_ref[...], NT, preferred_element_type=f32).astype(bf16)
    do_ref[...] = val
    dot_ref[...] = val.T


def dout_proj(g, w, bt=512):
    t, d = g.shape
    e = w.shape[0]
    return pl.pallas_call(
        dout_kernel,
        grid=(t // bt,),
        in_specs=[pl.BlockSpec((bt, d), lambda i: (i, 0)), pl.BlockSpec((e, d), lambda i: (0, 0))],
        out_specs=[pl.BlockSpec((bt, e), lambda i: (i, 0)), pl.BlockSpec((e, bt), lambda i: (0, i))],
        out_shape=[jax.ShapeDtypeStruct((t, e), bf16), jax.ShapeDtypeStruct((e, t), bf16)],
        compiler_params=pltpu.CompilerParams(vmem_limit_bytes=VMEM_LIMIT, dimension_semantics=("arbitrary",)),
        cost_estimate=pl.CostEstimate(flops=2 * t * d * e, bytes_accessed=2 * t * d, transcendentals=0),
        name="dout_proj")(g, w)


def fwd_kernel(q_ref, k_ref, vt_ref, o_ref, lse_ref, acc, ml, *, bq, bk, nh):
    i = pl.program_id(0)
    for h in range(nh):
        ml[2 * h:2 * h + 1, :] = jnp.full((1, bq), -1e30, f32)
        ml[2 * h + 1:2 * h + 2, :] = jnp.zeros((1, bq), f32)
    acc[...] = jnp.zeros_like(acc)

    def step(off, diag):
        kb = k_ref[pl.ds(off, bk), :]
        vt = vt_ref[:, pl.ds(off, bk)]
        if diag is not None:
            ki = lax.broadcasted_iota(jnp.int32, (bk, bq), 0) + diag
            qi = lax.broadcasted_iota(jnp.int32, (bk, bq), 1)
            keep = ki <= qi
        ss = [lax.dot_general(kb, q_ref[:, h * D:(h + 1) * D], NT, preferred_element_type=f32) for h in range(nh)]
        for h in range(nh):
            s = ss[h]
            if diag is not None:
                s = jnp.where(keep, s, -1e30)
            m_old = ml[2 * h:2 * h + 1, :]
            m_new = jnp.maximum(m_old, jnp.max(s, axis=0, keepdims=True))
            p = jnp.exp2(s * SCALE2 - m_new * SCALE2)
            alpha = jnp.exp2((m_old - m_new) * SCALE2)
            ml[2 * h:2 * h + 1, :] = m_new
            ml[2 * h + 1:2 * h + 2, :] = ml[2 * h + 1:2 * h + 2, :] * alpha + jnp.sum(p, axis=0, keepdims=True)
            pv = jnp.dot(vt, p.astype(bf16), preferred_element_type=f32)
            acc[h * D:(h + 1) * D, :] = acc[h * D:(h + 1) * D, :] * alpha + pv

    ratio = bq // bk

    def body(j, carry):
        step(pl.multiple_of(j * bk, bk), None)
        return carry

    lax.fori_loop(0, i * ratio, body, 0)
    for d in range(ratio):
        step(pl.multiple_of(i * bq + d * bk, bk), d * bk)
    for h in range(nh):
        m = ml[2 * h:2 * h + 1, :]
        l = ml[2 * h + 1:2 * h + 2, :]
        out_t = acc[h * D:(h + 1) * D, :] * (1.0 / l)
        o_ref[:, h * D:(h + 1) * D] = out_t.T.astype(bf16)
        lse_ref[:, h * D:(h + 1) * D] = jnp.broadcast_to(m * SCALE2 + jnp.log2(l), (D, bq)).T


def attn_fwd(q, k, vt, bq=1024, bk=512):
    t, e = q.shape
    nh = e // D
    row = pl.BlockSpec((bq, e), lambda i: (i, 0))
    return pl.pallas_call(
        functools.partial(fwd_kernel, bq=bq, bk=bk, nh=nh),
        grid=(t // bq,),
        in_specs=[row, pl.BlockSpec((t, D), lambda i: (0, 0)), pl.BlockSpec((D, t), lambda i: (0, 0))],
        out_specs=[row, row],
        out_shape=[jax.ShapeDtypeStruct((t, e), bf16), jax.ShapeDtypeStruct((t, e), f32)],
        scratch_shapes=[pltpu.VMEM((e, bq), f32), pltpu.VMEM((8, bq), f32)],
        compiler_params=pltpu.CompilerParams(vmem_limit_bytes=VMEM_LIMIT, dimension_semantics=("arbitrary",)),
        cost_estimate=pl.CostEstimate(flops=4 * t * t * e, bytes_accessed=8 * t * e, transcendentals=0),
        name="attn_fwd")(q, k, vt)


def peer_of(me, rel):
    bits = [me % 2, (me // 2) % 2, me // 4]
    flip = [rel % 2, (rel // 2) % 2, rel // 4]
    out = 0
    for n in range(3):
        bit = 1 - bits[n] if flip[n] else bits[n]
        out = out + bit * (1 << n)
    return out


def remote(src, dst, sems, slot, target):
    return pltpu.make_async_remote_copy(
        src_ref=src, dst_ref=dst, send_sem=sems[0].at[slot], recv_sem=sems[1].at[slot],
        device_id={'sp': target}, device_id_type=pl.DeviceIdType.MESH)


def meet_peers(me, n_dev):
    barrier = pltpu.get_barrier_semaphore()
    for rel in range(1, n_dev):
        pl.semaphore_signal(barrier, inc=1, device_id={'sp': peer_of(me, rel)}, device_id_type=pl.DeviceIdType.MESH)
    pl.semaphore_wait(barrier, n_dev - 1)


def bwd_kernel(q_ref, qt_ref, do_ref, dot_ref, o_ref, lse_ref, k_ref, v_ref, cos_ref, sin_ref, o_all,
               g_own, o_tok, g_tok, dlt, dqa, dka, dva, gqs, gks, gvs, loc_sem, o_send, o_recv, g_send, g_recv,
               *, bq, bk, t, nh, n_dev):
    h = pl.program_id(0)
    j = pl.program_id(1)
    nj = t // bk
    nq = t // bq
    rep = bk // D
    rows = t // n_dev
    early = nh - 1
    koff = pl.multiple_of(j * bk, bk)
    kc = pl.ds(koff, bk)
    me = lax.axis_index('sp')

    def rows_of(dev):
        return pl.ds(pl.multiple_of(dev * rows, rows), rows)

    def o_copy(rel):
        peer = peer_of(me, rel)
        return remote(o_all.at[rows_of(peer)], o_tok.at[me], (o_send, o_recv), rel - 1, peer)

    def g_copy(head, rel):
        peer = peer_of(me, rel)
        return remote(gqs.at[head, rows_of(peer)], g_tok.at[me, :, pl.ds(head * D, D)],
                      (g_send.at[head], g_recv.at[head]), rel - 1, peer)

    def o_local():
        return pltpu.make_async_copy(o_all.at[rows_of(me)], o_tok.at[me], loc_sem.at[0])

    def gq_local(head):
        return pltpu.make_async_copy(gqs.at[head], g_own.at[:, pl.ds(head * D, D)], loc_sem.at[1 + head])

    def gk_local(jj):
        r = pl.ds(jj * bk, bk)
        return pltpu.make_async_copy(gks.at[r], g_own.at[r, pl.ds(nh * D, D)], loc_sem.at[1 + nh + jj])

    def gv_local(jj):
        r = pl.ds(jj * bk, bk)
        return pltpu.make_async_copy(gvs.at[r], g_own.at[r, pl.ds((nh + 1) * D, D)], loc_sem.at[1 + nh + nj + jj])

    @pl.when((h == 0) & (j == 0))
    def _():
        meet_peers(me, n_dev)
        for rel in range(1, n_dev):
            o_copy(rel).start()
        o_local().start()

    @pl.when(j == 0)
    def _():
        def init(i, carry):
            r = pl.ds(pl.multiple_of(i * bq, bq), bq)
            d = jnp.sum(do_ref[r, :].astype(f32) * o_ref[r, :].astype(f32), axis=1, keepdims=True)
            dlt[r, :] = jnp.broadcast_to(d, (bq, D))
            dqa[r, :] = jnp.zeros((bq, D), f32)
            return carry
        lax.fori_loop(0, nq, init, 0)

    @pl.when(h == 0)
    def _():
        dka[:, kc] = jnp.zeros((D, bk), f32)
        dva[:, kc] = jnp.zeros((D, bk), f32)

    kb = k_ref[...]
    vb = v_ref[...]

    def step(i, diag):
        off = pl.multiple_of(i * bq, bq)
        r = pl.ds(off, bq)
        s = lax.dot_general(q_ref[r, :], kb, NT, preferred_element_type=f32)
        dp = lax.dot_general(do_ref[r, :], vb, NT, preferred_element_type=f32)
        if diag:
            qi = lax.broadcasted_iota(jnp.int32, (bq, bk), 0) + (off - koff)
            ki = lax.broadcasted_iota(jnp.int32, (bq, bk), 1)
            s = jnp.where(ki <= qi, s, -1e30)
        p = jnp.exp2(s * SCALE2 - jnp.concatenate([lse_ref[r, :]] * rep, axis=1))
        ds = ((dp - jnp.concatenate([dlt[r, :]] * rep, axis=1)) * p * SCALE).astype(bf16)
        dva[:, kc] += jnp.dot(dot_ref[:, r], p.astype(bf16), preferred_element_type=f32)
        dka[:, kc] += jnp.dot(qt_ref[:, r], ds, preferred_element_type=f32)
        dqa[r, :] += jnp.dot(ds, kb, preferred_element_type=f32)

    ratio = max(bk // bq, 1)
    first = (j * bk) // bq
    for d in range(ratio):
        step(first + d, True)

    def body(i, carry):
        step(i, False)
        return carry

    lax.fori_loop(first + ratio, nq, body, 0)

    for head in range(nh):
        @pl.when((j == nj - 1) & (h == head))
        def _():
            def fin(i, carry):
                r = pl.ds(pl.multiple_of(i * bq, bq), bq)
                dq = dqa[r, :].astype(bf16).astype(f32)
                gqs[head, r, :] = rotate(dq, cos_ref[r, :], -sin_ref[r, :]).astype(bf16)
                return carry
            lax.fori_loop(0, nq, fin, 0)
            gq_local(head).start()
            if head < early:
                for rel in range(1, n_dev):
                    g_copy(head, rel).start()

    for jj in range(nj):
        @pl.when((h == nh - 1) & (j == jj))
        def _():
            dk = dka[:, jj * bk:(jj + 1) * bk].T.astype(bf16).astype(f32)
            r = slice(jj * bk, (jj + 1) * bk)
            gks[r, :] = rotate(dk, cos_ref[r, :], -sin_ref[r, :]).astype(bf16)
            gvs[r, :] = dva[:, jj * bk:(jj + 1) * bk].T.astype(bf16)
            gk_local(jj).start()
            gv_local(jj).start()

    @pl.when((h == nh - 1) & (j == nj - 1))
    def _():
        o_local().wait()
        for head in range(nh):
            gq_local(head).wait()
        for jj in range(nj):
            gk_local(jj).wait()
            gv_local(jj).wait()
        for rel in range(1, n_dev):
            o_copy(rel).wait()
            for head in range(early):
                g_copy(head, rel).wait()


def attn_bwd(q, qt, do, dot, o, lse, k, v, cos, sin, n_dev, bq=512, bk=1024):
    t, e = q.shape
    nh = e // D
    nj = t // bk
    rows = t // n_dev
    col = pl.BlockSpec((t, D), lambda h, j: (0, h))
    row_t = pl.BlockSpec((D, t), lambda h, j: (h, 0))
    kv_in = pl.BlockSpec((bk, D), lambda h, j: (j, 0))
    table = pl.BlockSpec((t, D), lambda h, j: (0, 0), pipeline_mode=pl.Buffered(1))
    hbm = pl.BlockSpec(memory_space=pltpu.HBM)
    dma = pltpu.SemaphoreType.DMA
    return pl.pallas_call(
        functools.partial(bwd_kernel, bq=bq, bk=bk, t=t, nh=nh, n_dev=n_dev),
        grid=(nh, nj),
        in_specs=[col, row_t, col, row_t, col, col, kv_in, kv_in, table, table, hbm],
        out_specs=[hbm, hbm, hbm],
        out_shape=[jax.ShapeDtypeStruct((t, e + 2 * D), bf16), jax.ShapeDtypeStruct((n_dev, rows, e), bf16),
                   jax.ShapeDtypeStruct((n_dev, rows, (nh - 1) * D), bf16)],
        scratch_shapes=[pltpu.VMEM((t, D), f32), pltpu.VMEM((t, D), f32), pltpu.VMEM((D, t), f32), pltpu.VMEM((D, t), f32),
                        pltpu.VMEM((nh, t, D), bf16), pltpu.VMEM((t, D), bf16), pltpu.VMEM((t, D), bf16),
                        dma((1 + nh + 2 * nj,)), dma((n_dev - 1,)), dma((n_dev - 1,)), dma((nh - 1, n_dev - 1)), dma((nh - 1, n_dev - 1))],
        compiler_params=pltpu.CompilerParams(vmem_limit_bytes=VMEM_LIMIT, dimension_semantics=("arbitrary", "arbitrary"),
                                             collective_id=0, has_side_effects=True),
        cost_estimate=pl.CostEstimate(flops=10 * t * t * e, bytes_accessed=20 * t * e, transcendentals=0),
        name="attn_bwd")(q, qt, do, dot, o, lse, k, v, cos, sin, o)


N_CHUNK = 6
K_STEP = 4
N_COL = 12
N_ROW = 6


def tail_kernel(h_ref, g_vm, wo_ref, wq_ref, wk_ref, wv_ref, x_ref, lnw_ref, g_own, g_tok, o_tok,
                a_ref, dx_ref, dl_ref, dw_all, g_late,
                gt, acc, stage, lhs, dh, dlw, a2a_send, a2a_recv, ag_send, ag_recv, dl_send, dl_recv, st_sem, lhs_sem,
                *, n_dev):
    step = pl.program_id(0)
    me = lax.axis_index('sp')
    t, width = g_vm.shape
    rows = t // n_dev
    qe = width - 2 * D
    early = g_tok.shape[2]
    late = width - early
    dim = x_ref.shape[1]
    chunk = dim // N_CHUNK
    kk = t // K_STEP
    s_a = N_CHUNK * K_STEP
    s_dh = s_a + N_COL
    s_ln = s_dh + N_COL
    cw = dim // N_COL
    last = s_ln + N_ROW - 1
    peers = [me] + [peer_of(me, rel) for rel in range(1, n_dev)]
    SIB, XN, YN, DIAG = 1, 2, 4, 6

    def rows_of(dev):
        return pl.ds(pl.multiple_of(dev * rows, rows), rows)

    def late_copy(rel):
        return remote(g_own.at[rows_of(peers[rel]), pl.ds(early, late)], g_late.at[me], (a2a_send, a2a_recv), rel - 1, peers[rel])

    def piece(owner, n):
        return dw_all.at[pl.ds(pl.multiple_of(owner * dim + n * chunk, chunk), chunk)]

    def ag_copy(kind, n):
        owner, target = [(0, XN), (0, YN), (0, SIB), ((XN, YN) if n % 2 == 0 else (YN, XN)),
                         (XN, SIB), (YN, SIB), (DIAG, SIB)][kind]
        return remote(piece(peers[owner], n), piece(peers[owner], n), (ag_send.at[kind], ag_recv.at[kind]), n, peers[target])

    def dl_copy(rel):
        return remote(dlw.at[me], dlw.at[me], (dl_send, dl_recv), rel - 1, peers[rel])

    def store_chunk(n):
        return pltpu.make_async_copy(stage.at[n % 2], piece(me, n), st_sem.at[n % 2])

    def o_load(rel):
        src = peers[rel]
        return pltpu.make_async_copy(o_tok.at[src], lhs.at[:, pl.ds(pl.multiple_of(src * qe, D), qe)], lhs_sem.at[0, rel])

    def g_load(rel):
        src = peers[rel]
        if rel == 0:
            first, second, base = g_own.at[rows_of(me), pl.ds(0, early)], g_own.at[rows_of(me)], early
        else:
            first, second, base = g_tok.at[src], g_late.at[src], 0
        n_q = qe - early
        col = pl.multiple_of(src * qe, D)
        kcol = pl.multiple_of(dim + src * D, D)
        vcol = pl.multiple_of(dim + n_dev * D + src * D, D)
        return [pltpu.make_async_copy(first, lhs.at[:, pl.ds(col, early)], lhs_sem.at[1, rel]),
                pltpu.make_async_copy(second.at[:, pl.ds(base, n_q)], lhs.at[:, pl.ds(col + early, n_q)], lhs_sem.at[2, rel]),
                pltpu.make_async_copy(second.at[:, pl.ds(base + n_q, D)], lhs.at[:, pl.ds(kcol, D)], lhs_sem.at[3, rel]),
                pltpu.make_async_copy(second.at[:, pl.ds(base + n_q + D, D)], lhs.at[:, pl.ds(vcol, D)], lhs_sem.at[4, rel])]

    @pl.when(step == 0)
    def _():
        meet_peers(me, n_dev)
        for rel in (6, 7, 2, 4, 3, 5, 1):
            late_copy(rel).start()
        for rel in range(n_dev):
            o_load(rel).start()

        def flip(i, carry):
            r = pl.ds(pl.multiple_of(i * 512, 512), 512)
            gt[:, r] = g_vm[r, :].T
            return carry
        lax.fori_loop(0, t // 512, flip, 0)

    for n in range(N_CHUNK):
        @pl.when(step == (n + 1) * K_STEP)
        def _():
            store_chunk(n).wait()
            for kind in range(3):
                ag_copy(kind, n).start()

    @pl.when(step < s_a)
    def _():
        k = step % K_STEP
        part = jnp.dot(gt[:, pl.ds(pl.multiple_of(k * kk, kk), kk)], h_ref[...], preferred_element_type=f32)

        @pl.when(k == 0)
        def _():
            acc[...] = part

        @pl.when(k > 0)
        def _():
            acc[...] += part

    for n in range(N_CHUNK):
        @pl.when(step == (n + 1) * K_STEP - 1)
        def _():
            stage[n % 2] = acc[...].T.astype(bf16)
            store_chunk(n).start()

    @pl.when(step == s_a)
    def _():
        for rel in range(n_dev):
            o_load(rel).wait()

    @pl.when((step >= s_a) & (step < s_dh))
    def _():
        a_ref[...] = jnp.dot(lhs[:, :dim], wo_ref[...], preferred_element_type=f32).astype(bf16)

    @pl.when(step == s_dh)
    def _():
        for rel in range(1, n_dev):
            late_copy(rel).wait_recv()
        for rel in range(n_dev):
            for copy in g_load(rel):
                copy.start()
        for rel in range(n_dev):
            for copy in g_load(rel):
                copy.wait()

    for n in range(N_COL):
        @pl.when(step == s_dh + n)
        def _():
            kv = n_dev * D
            dh[:, n * cw:(n + 1) * cw] = (
                lax.dot_general(lhs[:, :dim], wq_ref[...], NT, preferred_element_type=f32)
                + lax.dot_general(lhs[:, dim:dim + kv], wk_ref[...], NT, preferred_element_type=f32)
                + lax.dot_general(lhs[:, dim + kv:], wv_ref[...], NT, preferred_element_type=f32))

    @pl.when(step >= s_ln)
    def _():
        n = step - s_ln
        br = rows // N_ROW
        x = x_ref[...].astype(f32)
        grad = dh[pl.ds(pl.multiple_of(n * br, br), br), :]
        cen = x - jnp.mean(x, axis=1, keepdims=True)
        rstd = lax.rsqrt(jnp.mean(cen * cen, axis=1, keepdims=True) + LN_EPS)
        xhat = cen * rstd
        dy = grad * lnw_ref[...].astype(f32)
        m1 = jnp.mean(dy, axis=1, keepdims=True)
        m2 = jnp.mean(dy * xhat, axis=1, keepdims=True)
        dx_ref[...] = (rstd * (dy - m1 - xhat * m2)).astype(bf16)
        part = jnp.sum((grad * xhat).reshape(br // 8, 8, dim), axis=0)

        @pl.when(n == 0)
        def _():
            dlw[me] = part

        @pl.when(n > 0)
        def _():
            dlw[me] += part

    @pl.when(step == last)
    def _():
        for rel in range(1, n_dev):
            dl_copy(rel).start()
        for n in range(N_CHUNK):
            ag_copy(0, n).wait_recv()
            if n % 2 == 0:
                ag_copy(3, n).start()
            ag_copy(4, n).start()
            ag_copy(1, n).wait_recv()
            if n % 2 == 1:
                ag_copy(3, n).start()
            ag_copy(5, n).start()
        for n in range(N_CHUNK):
            ag_copy(3, n).wait_recv()
            ag_copy(6, n).start()
        for rel in range(1, n_dev):
            dl_copy(rel).wait()
            late_copy(rel).wait_send()
        total = dlw[0]
        for dev in range(1, n_dev):
            total = total + dlw[dev]
        dl_ref[...] = jnp.sum(total, axis=0, keepdims=True).astype(bf16)
        for n in range(N_CHUNK):
            for kind in (2, 4, 5, 6):
                ag_copy(kind, n).wait_recv()
        for n in range(N_CHUNK):
            for kind in range(7):
                ag_copy(kind, n).wait_send()


def tail(h_all, g_own, g_tok, o_tok, w_o, w_q, w_k, w_v, x, lnw, n_dev):
    t, dim = h_all.shape
    width = g_own.shape[1]
    rows = t // n_dev
    s_a = N_CHUNK * K_STEP
    s_dh = s_a + N_COL
    s_ln = s_dh + N_COL
    chunk, cw, br = dim // N_CHUNK, dim // N_COL, rows // N_ROW
    early = g_tok.shape[2]
    kv = w_k.shape[1]
    hbm = pl.BlockSpec(memory_space=pltpu.HBM)
    dma = pltpu.SemaphoreType.DMA

    def h_map(s):
        c = jnp.minimum(s, s_a - 1)
        return c % K_STEP, c // K_STEP

    def at(first, count):
        return lambda s: jnp.clip(s - first, 0, count - 1)

    col_a, col_h, row_l = at(s_a, N_COL), at(s_dh, N_COL), at(s_ln, N_ROW)
    return pl.pallas_call(
        functools.partial(tail_kernel, n_dev=n_dev),
        grid=(s_ln + N_ROW,),
        in_specs=[pl.BlockSpec((t // K_STEP, chunk), h_map),
                  pl.BlockSpec((t, width), lambda s: (0, 0), pipeline_mode=pl.Buffered(1)),
                  pl.BlockSpec((dim, cw), lambda s: (0, col_a(s))),
                  pl.BlockSpec((cw, dim), lambda s: (col_h(s), 0)),
                  pl.BlockSpec((cw, kv), lambda s: (col_h(s), 0)),
                  pl.BlockSpec((cw, kv), lambda s: (col_h(s), 0)),
                  pl.BlockSpec((br, dim), lambda s: (row_l(s), 0)),
                  pl.BlockSpec((1, dim), lambda s: (0, 0)),
                  hbm, hbm, hbm],
        out_specs=[pl.BlockSpec((rows, cw), lambda s: (0, col_a(s))),
                   pl.BlockSpec((br, dim), lambda s: (row_l(s), 0)),
                   pl.BlockSpec((1, dim), lambda s: (0, 0)),
                   hbm, hbm],
        out_shape=[jax.ShapeDtypeStruct((rows, dim), bf16), jax.ShapeDtypeStruct((rows, dim), bf16),
                   jax.ShapeDtypeStruct((1, dim), bf16), jax.ShapeDtypeStruct((n_dev * dim, width), bf16),
                   jax.ShapeDtypeStruct((n_dev, rows, width - early), bf16)],
        scratch_shapes=[pltpu.VMEM((width, t), bf16), pltpu.VMEM((width, chunk), f32), pltpu.VMEM((2, chunk, width), bf16),
                        pltpu.VMEM((rows, dim + 2 * kv), bf16), pltpu.VMEM((rows, dim), f32), pltpu.VMEM((n_dev, 8, dim), f32),
                        dma((n_dev - 1,)), dma((n_dev - 1,)), dma((7, N_CHUNK)), dma((7, N_CHUNK)),
                        dma((n_dev - 1,)), dma((n_dev - 1,)), dma((2,)), dma((5, n_dev))],
        compiler_params=pltpu.CompilerParams(vmem_limit_bytes=VMEM_LIMIT, dimension_semantics=("arbitrary",),
                                             collective_id=1, has_side_effects=True),
        name="tail")(h_all, g_own, w_o, w_q, w_k, w_v, x, lnw, g_own, g_tok, o_tok)


def spread_kernel(src_ref, q_ref, k_ref, v_ref):
    n_dev, _, width = src_ref.shape
    qe = width - 2 * D
    for dev in range(n_dev):
        q_ref[:, dev * qe:(dev + 1) * qe] = src_ref[dev, :, :qe]
        k_ref[:, dev * D:(dev + 1) * D] = src_ref[dev, :, qe:qe + D]
        v_ref[:, dev * D:(dev + 1) * D] = src_ref[dev, :, qe + D:]


def spread(dw_all, bt=256):
    n_dev, dim, width = dw_all.shape
    qe = width - 2 * D
    return pl.pallas_call(
        spread_kernel,
        grid=(dim // bt,),
        in_specs=[pl.BlockSpec((n_dev, bt, width), lambda i: (0, i, 0))],
        out_specs=[pl.BlockSpec((bt, n_dev * c), lambda i: (i, 0)) for c in (qe, D, D)],
        out_shape=[jax.ShapeDtypeStruct((dim, n_dev * c), bf16) for c in (qe, D, D)],
        compiler_params=pltpu.CompilerParams(vmem_limit_bytes=VMEM_LIMIT, dimension_semantics=("arbitrary",)),
        name="spread")(dw_all)


def norm_f32(hid_f32, weight_f32):
    mean_val = jnp.mean(hid_f32, axis=-1, keepdims=True)
    centered = hid_f32 - mean_val
    var_val = jnp.mean(centered * centered, axis=-1, keepdims=True)
    return centered * lax.rsqrt(var_val + LN_EPS) * weight_f32


def rope_tables(positions):
    lane = jnp.arange(D, dtype=jnp.int32)
    inv_freq = ROPE_BASE ** (-(lane - lane % 2).astype(f32) / D)
    angles = positions.astype(f32)[:, None] * inv_freq[None, :]
    sin = jnp.sin(angles)
    return jnp.cos(angles), jnp.where(lane[None, :] % 2 == 0, -sin, sin)


def solution(mesh):
    n_dev = mesh.shape['sp']
    row_spec = P(('dp', 'sp'), None)
    pos_spec = P(('dp', 'sp'))
    full_spec = P(None, None)
    grad_spec = P('dp', None)

    def local_step(hidden, positions, d_attn, ln_weight, w_q, w_k, w_v, w_o):
        rows, dim = hidden.shape
        idx = lax.axis_index('sp')
        qe = w_q.shape[1] // n_dev
        ke = w_k.shape[1] // n_dev
        normed = norm_f32(hidden.astype(f32), ln_weight.astype(f32)).astype(bf16)
        h_all = lax.all_gather(normed, 'sp', axis=0, tiled=True)
        g_all = lax.all_gather(d_attn, 'sp', axis=0, tiled=True)
        cos, sin = rope_tables(lax.all_gather(positions, 'sp', axis=0, tiled=True))
        w_own = jnp.concatenate([lax.dynamic_slice_in_dim(w_q, idx * qe, qe, 1), lax.dynamic_slice_in_dim(w_k, idx * ke, ke, 1),
                                 lax.dynamic_slice_in_dim(w_v, idx * ke, ke, 1)], axis=1)
        wo_own = lax.dynamic_slice_in_dim(w_o, idx * qe, qe, 0)
        q, qt, k, v, vt = project(h_all, w_own, cos, sin, qe // D)
        o, lse = attn_fwd(q, k, vt)
        do, dot = dout_proj(g_all, wo_own)
        dwo_own = jnp.einsum('te,td->ed', o, g_all, preferred_element_type=f32).astype(bf16)
        dw_o = lax.all_gather(dwo_own, 'sp', axis=0, tiled=True)
        g_own, o_tok, g_tok = attn_bwd(q, qt, do, dot, o, lse, k, v, cos, sin, n_dev)
        attn_out, d_hid, d_lnw, dw_all, _ = tail(h_all, g_own, g_tok, o_tok, w_o, w_q, w_k, w_v, hidden,
                                                 ln_weight.reshape(1, dim), n_dev)
        dw_q, dw_k, dw_v = spread(dw_all.reshape(n_dev, dim, qe + 2 * ke))
        return attn_out, d_hid, d_lnw.reshape(dim), dw_q, dw_k, dw_v, dw_o

    return jax.shard_map(local_step, mesh=mesh,
                         in_specs=(row_spec, pos_spec, row_spec, P(None), full_spec, full_spec, full_spec, full_spec),
                         out_specs=(row_spec, row_spec, P('dp'), grad_spec, grad_spec, grad_spec, grad_spec),
                         check_vma=False)
```

```python
import functools
import math
import jax
import jax.numpy as jnp
from jax import lax
from jax.experimental import pallas as pl
from jax.experimental.pallas import tpu as pltpu
from jax.sharding import PartitionSpec as P

D = 128
LN_EPS = 1e-5
ROPE_BASE = 10000.0
SCALE = D ** -0.5
SCALE2 = SCALE * math.log2(math.e)
NT = (((1,), (1,)), ((), ()))
f32 = jnp.float32
bf16 = jnp.bfloat16
VMEM_LIMIT = 60 * 2 ** 20
shape = jax.ShapeDtypeStruct
dma = pltpu.SemaphoreType.DMA
hbm = pl.BlockSpec(memory_space=pltpu.HBM)


def params(axes=1, **more):
    more.update(has_side_effects=bool(more))
    return pltpu.CompilerParams(vmem_limit_bytes=VMEM_LIMIT, dimension_semantics=("arbitrary",) * axes, **more)


def fixed(i):
    return 0, 0


def rows_at(i):
    return i, 0


def cols_at(i):
    return 0, i


def others(n_dev):
    return range(1, n_dev)


def lanes(h):
    return slice(h * D, (h + 1) * D)


def norm_f32(hid_f32, weight_f32):
    mean_val = jnp.mean(hid_f32, axis=-1, keepdims=True)
    centered = hid_f32 - mean_val
    var_val = jnp.mean(centered * centered, axis=-1, keepdims=True)
    return centered * lax.rsqrt(var_val + LN_EPS) * weight_f32


SIB, XN, YN, DIAG = 1, 2, 4, 6


def peer_of(me, rel):
    mine = (me % 2, (me // 2) % 2, me // 4)
    flip = (rel % 2, (rel // 2) % 2, rel // 4)
    return sum(((mine[n] + flip[n]) % 2) * (1 << n) for n in range(3))


def remote(src, dst, sems, slot, target):
    return pltpu.make_async_remote_copy(
        src_ref=src, dst_ref=dst, send_sem=sems[0].at[slot], recv_sem=sems[1].at[slot],
        device_id={'sp': target}, device_id_type=pl.DeviceIdType.MESH)


def meet_peers(me, n_dev):
    barrier = pltpu.get_barrier_semaphore()
    for rel in others(n_dev):
        pl.semaphore_signal(barrier, device_id={'sp': peer_of(me, rel)}, device_id_type=pl.DeviceIdType.MESH)
    pl.semaphore_wait(barrier, n_dev - 1)


def gather_copy(kind, n, own, piece, sems, me):
    if kind == 3:
        owner, target = (XN, YN) if n % 2 == 0 else (YN, XN)
    else:
        owner, target = {0: (0, XN), 1: (0, YN), 2: (0, SIB), 4: (XN, SIB), 5: (YN, SIB), 6: (DIAG, SIB)}[kind]
    dst = piece(peer_of(me, owner), n)
    return remote(own(n) if owner == 0 else dst, dst, (sems[0].at[kind], sems[1].at[kind]), n, peer_of(me, target))


def rotate(val, cos, sin):
    even = lax.rem(lax.broadcasted_iota(jnp.int32, val.shape, 1), 2) == 0
    swapped = jnp.where(even, pltpu.roll(val, D - 1, 1), pltpu.roll(val, 1, 1))
    return val * cos + swapped * sin


N_SUB = 3


def item_of(s, n_dev):
    n_mid = 4 * N_SUB
    first = 2 * N_SUB
    u, w = s - first, s - first - n_mid
    r = u % 4
    rel = jnp.where(s < first, s // N_SUB, jnp.where(s < first + n_mid, 2 + 2 * (r % 2) + r // 2, 6 + w % 2))
    m = jnp.where(s < first, s % N_SUB, jnp.where(s < first + n_mid, u // 4, w // 2))
    return rel, m


def items(n_dev):
    out = [(rel, m) for rel in (0, SIB) for m in range(N_SUB)]
    out += [(rel, m) for m in range(N_SUB) for rel in (XN, YN, XN + 1, YN + 1)]
    return out + [(rel, m) for m in range(N_SUB) for rel in (DIAG, DIAG + 1)]


def start_kernel(x_ref, lnw_ref, wq_hbm, wk_hbm, wv_hbm, freq_ref, pos_ref, q_ref, qt_ref, k_ref, v_ref, vt_ref, cos_ref, sin_ref, h_all,
                 w_ref, hs, buf, pos_all, w_sem, loc_sem, ld_sem, pos_send, pos_recv, ag_send, ag_recv, *, n_dev, nh):
    step = pl.program_id(0)
    me = lax.axis_index('sp')
    rows = x_ref.shape[0]
    size = rows // (2 * N_SUB)
    sub = 2 * size
    order = items(n_dev)
    rel_t, m_t = item_of(step, n_dev)
    owner_t = peer_of(me, rel_t)

    def own(n):
        return hs.at[pl.ds(pl.multiple_of(n * size, size), size)]

    def piece(owner, n):
        return h_all.at[pl.ds(pl.multiple_of(owner * rows + n * size, size), size)]

    def copy(kind, n):
        return gather_copy(kind, n, own, piece, (ag_send, ag_recv), me)

    def pos_copy(rel):
        return remote(pos_all.at[me], pos_all.at[me], (pos_send, pos_recv), rel, peer_of(me, rel))

    def keep_own():
        return pltpu.make_async_copy(hs, h_all.at[pl.ds(pl.multiple_of(me * rows, rows), rows)], loc_sem)

    def load(i):
        rel, m = order[i]
        src = h_all.at[pl.ds(pl.multiple_of(peer_of(me, rel) * rows + m * sub, sub), sub)]
        return pltpu.make_async_copy(src, buf.at[i % 2], ld_sem.at[i % 2])

    def arrive(i):
        rel, m = order[i]
        for n in (2 * m, 2 * m + 1):
            if rel == SIB:
                copy(2, n).wait_recv()
            elif rel in (XN, YN):
                copy(0 if rel == XN else 1, n).wait_recv()
                if (rel == XN) == (n % 2 == 0):
                    copy(3, n).start()
                copy(4 if rel == XN else 5, n).start()
            elif rel in (XN + 1, YN + 1):
                copy(4 if rel == XN + 1 else 5, n).wait_recv()
            elif rel == DIAG:
                copy(3, n).wait_recv()
                copy(6, n).start()
            elif rel == DIAG + 1:
                copy(6, n).wait_recv()

    def w_load(i):
        col, size_w, src = ((0, nh * D, wq_hbm), (nh * D, D, wk_hbm), ((nh + 1) * D, D, wv_hbm))[i]
        return pltpu.make_async_copy(src.at[:, pl.ds(pl.multiple_of(me * size_w, D), size_w)], w_ref.at[:, pl.ds(col, size_w)], w_sem.at[i])

    @pl.when(step == 0)
    def _():
        for i in range(3):
            w_load(i).start()
        pos_all[me] = pos_ref[:]
        meet_peers(me, n_dev)

        def norm(n, carry):
            r = pl.ds(pl.multiple_of(n * size, size), size)
            hs[r, :] = norm_f32(x_ref[r, :].astype(f32), lnw_ref[:].astype(f32)).astype(bf16)

            @pl.when(n > 0)
            def _():
                for kind in range(3):
                    copy(kind, n - 1).start()
            return carry
        lax.fori_loop(0, 2 * N_SUB, norm, 0)
        for rel in others(n_dev):
            pos_copy(rel).start()
        for kind in range(3):
            copy(kind, 2 * N_SUB - 1).start()
        keep_own().start()
        keep_own().wait()
        load(0).start()
        for i in range(3):
            w_load(i).wait()

    for i in range(1, len(order)):
        @pl.when(step == i - 1)
        def _():
            if i == N_SUB:
                for rel in others(n_dev):
                    pos_copy(rel).wait_recv()
            arrive(i)
            load(i).start()

    slot = step % 2
    pltpu.make_async_copy(h_all.at[pl.ds(0, sub)], buf.at[slot], ld_sem.at[slot]).wait()
    tile = pos_all[owner_t, m_t].astype(f32)
    pos = jnp.concatenate([jnp.broadcast_to(tile[i:i + 1, :], (D, D)).T for i in range(sub // D)], axis=0)
    angles = pos * freq_ref[:]
    cos = jnp.cos(angles)
    sin = jnp.sin(angles)
    sin = jnp.where(lax.rem(lax.broadcasted_iota(jnp.int32, sin.shape, 1), 2) == 0, -sin, sin)
    cos_ref[:] = cos
    sin_ref[:] = sin
    res = jnp.dot(buf[slot], w_ref[:], preferred_element_type=f32)
    for n in range(nh):
        rot = rotate(res[:, lanes(n)], cos, sin).astype(bf16)
        q_ref[:, lanes(n)] = rot
        qt_ref[lanes(n), :] = rot.T
    k_ref[:] = rotate(res[:, lanes(nh)], cos, sin).astype(bf16)
    v = res[:, (nh + 1) * D:].astype(bf16)
    v_ref[:] = v
    vt_ref[:] = v.T

    @pl.when(step == len(order) - 1)
    def _():
        for rel in others(n_dev):
            pos_copy(rel).wait_send()
        for n in range(2 * N_SUB):
            for kind in range(7):
                copy(kind, n).wait_send()


def start(x, lnw, w_q, w_k, w_v, freq, pos, nh, n_dev):
    rows, dim = x.shape
    t = rows * n_dev
    sub = rows // N_SUB
    whole = lambda a: pl.BlockSpec(a.shape, lambda s: (0,) * a.ndim, pipeline_mode=pl.Buffered(1))

    def at(s):
        rel, m = item_of(s, n_dev)
        return peer_of(lax.axis_index('sp'), rel) * N_SUB + m

    row = lambda c: pl.BlockSpec((sub, c), lambda s: (at(s), 0))
    col = lambda r: pl.BlockSpec((r, sub), lambda s: (0, at(s)))
    return pl.pallas_call(
        functools.partial(start_kernel, n_dev=n_dev, nh=nh),
        grid=(n_dev * N_SUB,),
        in_specs=[whole(x), whole(lnw), hbm, hbm, hbm, whole(freq), whole(pos)],
        out_specs=[row(nh * D), col(nh * D), row(D), row(D), col(D), row(D), row(D), hbm],
        out_shape=[shape((t, nh * D), bf16), shape((nh * D, t), bf16), shape((t, D), bf16), shape((t, D), bf16), shape((D, t), bf16),
                   shape((t, D), f32), shape((t, D), f32), shape((t, dim), bf16)],
        scratch_shapes=[pltpu.VMEM((dim, (nh + 2) * D), bf16), pltpu.VMEM((rows, dim), bf16), pltpu.VMEM((2, sub, dim), bf16),
                        pltpu.VMEM((n_dev,) + pos.shape, jnp.int32), dma((3,)), dma, dma((2,)), dma((n_dev,)), dma((n_dev,)), dma((7, 2 * N_SUB)), dma((7, 2 * N_SUB))],
        compiler_params=params(1, collective_id=4),
        name="start")(x, lnw, w_q, w_k, w_v, freq, pos)


def mid_kernel(g_blk, ot_ref, w_ref, g_own, do_ref, dot_ref, dwo_ref, g_rest, acc, buf, ld_sem, ag_send, ag_recv, *, n_dev, rows, first):
    step = pl.program_id(0)
    me = lax.axis_index('sp')
    rest = rows - first
    half = rest // 2
    order = (0, SIB, XN, YN, XN + 1, YN + 1, DIAG, DIAG + 1)

    def own(n):
        return g_own.at[pl.ds(first + n * half, half)]

    def piece(owner, n):
        return g_rest.at[pl.ds(pl.multiple_of(owner * rest + n * half, half), half)]

    def copy(kind, n):
        return gather_copy(kind, n, own, piece, (ag_send, ag_recv), me)

    def load(i):
        owner = peer_of(me, order[i])
        src = g_own.at[pl.ds(first, rest)] if i == 0 else g_rest.at[pl.ds(pl.multiple_of(owner * rest, rest), rest)]
        return pltpu.make_async_copy(src, buf.at[i % 2], ld_sem.at[i % 2])

    def compute(g, row0, size):
        r = pl.ds(row0, size)
        val = lax.dot_general(g, w_ref[:], NT, preferred_element_type=f32).astype(bf16)
        do_ref[r, :] = val
        dot_ref[:, r] = val.T
        acc[:] += jnp.dot(ot_ref[:, r], g, preferred_element_type=f32)

    @pl.when(step == 0)
    def _():
        meet_peers(me, n_dev)
        for n in range(2):
            for kind in range(3):
                copy(kind, n).start()
        acc[:] = jnp.zeros_like(acc)

    @pl.when(step == 5)
    def _():
        copy(0, 0).wait_recv()
        copy(3, 0).start()
        copy(4, 0).start()

    @pl.when(step == n_dev)
    def _():
        copy(1, 1).wait_recv()
        copy(3, 1).start()
        copy(5, 1).start()
        copy(0, 1).wait_recv()
        copy(4, 1).start()
        copy(1, 0).wait_recv()
        copy(5, 0).start()

    waits = {1: ((2, 0), (2, 1)), 4: ((4, 0), (4, 1)), 5: ((5, 0), (5, 1)), 6: ((3, 0), (3, 1)), 7: ((6, 0), (6, 1))}
    for i in range(n_dev):
        @pl.when(step == n_dev - 1 + i)
        def _():
            for kind, n in waits.get(i, ()):
                copy(kind, n).wait_recv()
                if kind == 3:
                    copy(6, n).start()
            load(i).start()

    @pl.when(step < n_dev)
    def _():
        compute(g_blk[:], pl.multiple_of(step * rows, D), first)

    for i in range(n_dev):
        @pl.when(step == n_dev + i)
        def _():
            load(i).wait()
            compute(buf[i % 2], pl.multiple_of(peer_of(me, order[i]) * rows + first, D), rest)

    @pl.when(step == 2 * n_dev - 1)
    def _():
        dwo_ref[:] = acc[:].astype(bf16)
        for n in range(2):
            for kind in range(7):
                copy(kind, n).wait_send()


def mid(g_first, ot, w, g_own, n_dev):
    dim = g_own.shape[1]
    rows = g_own.shape[0]
    first = g_first.shape[0] // n_dev
    rest = rows - first
    e, t = ot.shape
    whole = lambda a, b: pl.BlockSpec((a, b), fixed, pipeline_mode=pl.Buffered(1))
    const = lambda a, b: pl.BlockSpec((a, b), fixed)
    w_spec = pl.BlockSpec((e, dim), lambda i: (lax.axis_index('sp'), 0), pipeline_mode=pl.Buffered(1))
    return pl.pallas_call(
        functools.partial(mid_kernel, n_dev=n_dev, rows=rows, first=first),
        grid=(2 * n_dev,),
        in_specs=[pl.BlockSpec((first, dim), lambda i: (jnp.minimum(i, n_dev - 1), 0)), whole(e, t), w_spec, hbm],
        out_specs=[const(t, e), const(e, t), const(e, dim), hbm],
        out_shape=[shape((t, e), bf16), shape((e, t), bf16), shape((e, dim), bf16),
                   shape((n_dev * rest, dim), bf16)],
        scratch_shapes=[pltpu.VMEM((e, dim), f32), pltpu.VMEM((2, rest, dim), bf16), dma((2,)), dma((7, 2)), dma((7, 2))],
        compiler_params=params(1, collective_id=3),
        name="mid")(g_first, ot, w, g_own)


def fwd_kernel(q_ref, k_ref, vt_ref, g_own, o_ref, ot_ref, lse_ref, g_first, acc, m_ref, l_ref, loc_sem, ag_send, ag_recv,
               *, bq, bk, nh, n_dev, first, n_piece):
    i = pl.program_id(0)
    nq = pl.num_programs(0)
    me = lax.axis_index('sp')
    size = first // n_piece

    def own(n):
        return g_own.at[pl.ds(n * size, size)]

    def piece(owner, n):
        return g_first.at[pl.ds(pl.multiple_of(owner * first + n * size, size), size)]

    def copy(kind, n):
        return gather_copy(kind, n, own, piece, (ag_send, ag_recv), me)

    def keep_own():
        return pltpu.make_async_copy(g_own.at[pl.ds(0, first)], g_first.at[pl.ds(pl.multiple_of(me * first, first), first)], loc_sem)

    def pass_on(n):
        copy(0, n).wait_recv()
        copy(1, n).wait_recv()
        copy(3, n).start()
        copy(4, n).start()
        copy(5, n).start()

    @pl.when(i == 0)
    def _():
        meet_peers(me, n_dev)
        for n in range(n_piece):
            for kind in range(3):
                copy(kind, n).start()
        keep_own().start()

    @pl.when(i == nq - 2)
    def _():
        for n in range(n_piece // 2):
            pass_on(n)

    @pl.when(i == nq - 1)
    def _():
        for n in range(n_piece // 2, n_piece):
            pass_on(n)

    for h in range(nh):
        m_ref[h:h + 1, :] = jnp.full((1, bq), -1e30, f32)
        l_ref[h:h + 1, :] = jnp.zeros((1, bq), f32)
    acc[:] = jnp.zeros_like(acc)

    def step(off, diag):
        q0 = 0 if diag is None else diag
        kb = k_ref[pl.ds(off, bk), :]
        vt = vt_ref[:, pl.ds(off, bk)]
        if diag is not None:
            ki = lax.broadcasted_iota(jnp.int32, (bk, bq - q0), 0)
            qi = lax.broadcasted_iota(jnp.int32, (bk, bq - q0), 1)
            keep = ki <= qi
        ss = [lax.dot_general(kb, q_ref[q0:, lanes(h)], NT, preferred_element_type=f32) for h in range(nh)]
        for h in range(nh):
            s = ss[h]
            if diag is not None:
                s = jnp.where(keep, s, -1e30)
            m_old = m_ref[h:h + 1, q0:]
            m_new = jnp.maximum(m_old, jnp.max(s, axis=0, keepdims=True))
            p = jnp.exp2(s * SCALE2 - m_new * SCALE2)
            alpha = jnp.exp2((m_old - m_new) * SCALE2)
            m_ref[h:h + 1, q0:] = m_new
            l_ref[h:h + 1, q0:] = l_ref[h:h + 1, q0:] * alpha + jnp.sum(p, axis=0, keepdims=True)
            pv = jnp.dot(vt, p.astype(bf16), preferred_element_type=f32)
            acc[lanes(h), q0:] = acc[lanes(h), q0:] * alpha + pv

    ratio = bq // bk

    def body(j, carry):
        step(pl.multiple_of(j * bk, bk), None)
        return carry

    lax.fori_loop(0, i * ratio, body, 0)
    for d in range(ratio):
        step(pl.multiple_of(i * bq + d * bk, bk), d * bk)
    for h in range(nh):
        m = m_ref[h:h + 1, :]
        l = l_ref[h:h + 1, :]
        out_t = acc[lanes(h), :] * (1.0 / l)
        o_ref[:, lanes(h)] = out_t.T.astype(bf16)
        ot_ref[lanes(h), :] = out_t.astype(bf16)
        lse_ref[:, lanes(h)] = jnp.broadcast_to(m * SCALE2 + jnp.log2(l), (D, bq)).T

    @pl.when(i == nq - 1)
    def _():
        for n in range(n_piece):
            copy(3, n).wait_recv()
            copy(6, n).start()
        keep_own().wait()
        for n in range(n_piece):
            for kind in (2, 4, 5, 6):
                copy(kind, n).wait_recv()
            for kind in range(7):
                copy(kind, n).wait_send()


def attn_fwd(q, k, vt, g_own, first, n_dev, bq=1024, bk=512, n_piece=4):
    t, e = q.shape
    nh = e // D
    row = pl.BlockSpec((bq, e), rows_at)
    return pl.pallas_call(
        functools.partial(fwd_kernel, bq=bq, bk=bk, nh=nh, n_dev=n_dev, first=first, n_piece=n_piece),
        grid=(t // bq,),
        in_specs=[row, pl.BlockSpec((t, D), fixed), pl.BlockSpec((D, t), fixed), hbm],
        out_specs=[row, pl.BlockSpec((e, bq), cols_at), row, hbm],
        out_shape=[shape((t, e), bf16), shape((e, t), bf16), shape((t, e), f32),
                   shape((n_dev * first, g_own.shape[1]), bf16)],
        scratch_shapes=[pltpu.VMEM((e, bq), f32), pltpu.VMEM((8, bq), f32), pltpu.VMEM((8, bq), f32), dma, dma((7, n_piece)), dma((7, n_piece))],
        compiler_params=params(1, collective_id=2),
        name="attn_fwd")(q, k, vt, g_own)


def bwd_kernel(q_ref, qt_ref, do_ref, dot_ref, o_ref, lse_ref, k_ref, v_ref, cos_ref, sin_ref, o_all, dwo_own,
               g_own, o_tok, g_tok, dwo_all, dlt, dqa, dka, dva, gqs, gks, gvs, loc_sem, o_send, o_recv, g_send, g_recv,
               w_sem, ag_send, ag_recv, *, bq, bk, t, nh, n_dev):
    h = pl.program_id(0)
    j = pl.program_id(1)
    nj = t // bk
    nq = t // bq
    rep = bk // D
    rows = t // n_dev
    early = nh - 1
    koff = pl.multiple_of(j * bk, bk)
    kc = pl.ds(koff, bk)
    me = lax.axis_index('sp')

    def rows_of(dev):
        return pl.ds(pl.multiple_of(dev * rows, rows), rows)

    def o_copy(rel):
        peer = peer_of(me, rel)
        return remote(o_all.at[rows_of(peer)], o_tok.at[me], (o_send, o_recv), rel, peer)

    def g_copy(head, rel):
        peer = peer_of(me, rel)
        return remote(gqs.at[head, rows_of(peer)], g_tok.at[me, :, pl.ds(head * D, D)],
                      (g_send.at[head], g_recv.at[head]), rel, peer)

    half = dwo_own.shape[0] // 2

    def own(n):
        return dwo_own.at[pl.ds(n * half, half)]

    def piece(owner, n):
        return dwo_all.at[pl.ds(pl.multiple_of((2 * owner + n) * half, half), half)]

    def w_copy(kind, n):
        return gather_copy(kind, n, own, piece, (ag_send, ag_recv), me)

    def w_local(n):
        return pltpu.make_async_copy(own(n), piece(me, n), w_sem.at[n])

    def o_local():
        return pltpu.make_async_copy(o_all.at[rows_of(me)], o_tok.at[me], loc_sem.at[0])

    def gq_local(head):
        return pltpu.make_async_copy(gqs.at[head], g_own.at[:, pl.ds(head * D, D)], loc_sem.at[1 + head])

    def gk_local(jj):
        r = pl.ds(jj * bk, bk)
        return pltpu.make_async_copy(gks.at[r], g_own.at[r, pl.ds(nh * D, D)], loc_sem.at[1 + nh + jj])

    def gv_local(jj):
        r = pl.ds(jj * bk, bk)
        return pltpu.make_async_copy(gvs.at[r], g_own.at[r, pl.ds((nh + 1) * D, D)], loc_sem.at[1 + nh + nj + jj])

    @pl.when((h == 0) & (j == 0))
    def _():
        meet_peers(me, n_dev)
        for rel in others(n_dev):
            o_copy(rel).start()
        o_local().start()
        for n in range(2):
            w_local(n).start()
            for kind in range(3):
                w_copy(kind, n).start()

    @pl.when((h == nh - 1) & (j == 0))
    def _():
        for n in range(2):
            w_copy(0, n).wait_recv()
            w_copy(1, n).wait_recv()
            for kind in (3, 4, 5):
                w_copy(kind, n).start()

    @pl.when(j == 0)
    def _():
        def init(i, carry):
            r = pl.ds(pl.multiple_of(i * bq, bq), bq)
            d = jnp.sum(do_ref[r, :].astype(f32) * o_ref[r, :].astype(f32), axis=1, keepdims=True)
            dlt[r, :] = jnp.broadcast_to(d, (bq, D))
            dqa[r, :] = jnp.zeros((bq, D), f32)
            return carry
        lax.fori_loop(0, nq, init, 0)

    @pl.when(h == 0)
    def _():
        dka[:, kc] = jnp.zeros((D, bk), f32)
        dva[:, kc] = jnp.zeros((D, bk), f32)

    def step(i, diag):
        off = pl.multiple_of(i * bq, bq)
        r = pl.ds(off, bq)
        nk = bk if diag is None else diag + bq
        rep = nk // D
        kc = pl.ds(koff, nk)
        kb, vb = k_ref[:nk, :], v_ref[:nk, :]
        s = lax.dot_general(q_ref[r, :], kb, NT, preferred_element_type=f32)
        dp = lax.dot_general(do_ref[r, :], vb, NT, preferred_element_type=f32)
        if diag is not None:
            qi = lax.broadcasted_iota(jnp.int32, (bq, nk), 0) + diag
            ki = lax.broadcasted_iota(jnp.int32, (bq, nk), 1)
            s = jnp.where(ki <= qi, s, -1e30)
        p = jnp.exp2(s * SCALE2 - jnp.concatenate([lse_ref[r, :]] * rep, axis=1))
        ds = ((dp - jnp.concatenate([dlt[r, :]] * rep, axis=1)) * p * SCALE).astype(bf16)
        dva[:, kc] += jnp.dot(dot_ref[:, r], p.astype(bf16), preferred_element_type=f32)
        dka[:, kc] += jnp.dot(qt_ref[:, r], ds, preferred_element_type=f32)
        dqa[r, :] += jnp.dot(ds, kb, preferred_element_type=f32)

    ratio = max(bk // bq, 1)
    first = (j * bk) // bq
    for d in range(ratio):
        step(first + d, d * bq)

    def body(i, carry):
        step(i, None)
        return carry

    lax.fori_loop(first + ratio, nq, body, 0)

    for head in range(nh):
        @pl.when((j == nj - 1) & (h == head))
        def _():
            def fin(i, carry):
                r = pl.ds(pl.multiple_of(i * bq, bq), bq)
                dq = dqa[r, :].astype(bf16).astype(f32)
                gqs[head, r, :] = rotate(dq, cos_ref[r, :], -sin_ref[r, :]).astype(bf16)
                return carry
            lax.fori_loop(0, nq, fin, 0)
            gq_local(head).start()
            if head < early:
                for rel in others(n_dev):
                    g_copy(head, rel).start()

    for jj in range(nj):
        @pl.when((h == nh - 1) & (j == jj))
        def _():
            dk = dka[:, jj * bk:(jj + 1) * bk].T.astype(bf16).astype(f32)
            r = slice(jj * bk, (jj + 1) * bk)
            gks[r, :] = rotate(dk, cos_ref[r, :], -sin_ref[r, :]).astype(bf16)
            gvs[r, :] = dva[:, jj * bk:(jj + 1) * bk].T.astype(bf16)
            gk_local(jj).start()
            gv_local(jj).start()

    @pl.when((h == nh - 1) & (j == nj - 1))
    def _():
        for n in range(2):
            w_local(n).wait()
            w_copy(3, n).wait_recv()
            w_copy(6, n).start()
        o_local().wait()
        for head in range(nh):
            gq_local(head).wait()
        for jj in range(nj):
            gk_local(jj).wait()
            gv_local(jj).wait()
        for rel in others(n_dev):
            o_copy(rel).wait()
            for head in range(early):
                g_copy(head, rel).wait()
        for n in range(2):
            for kind in (2, 4, 5, 6):
                w_copy(kind, n).wait_recv()
            for kind in range(7):
                w_copy(kind, n).wait_send()


def attn_bwd(q, qt, do, dot, o, lse, k, v, cos, sin, dwo, n_dev, bq=512, bk=1024):
    t, e = q.shape
    nh = e // D
    nj = t // bk
    rows = t // n_dev
    col = pl.BlockSpec((t, D), lambda h, j: (0, h))
    row_t = pl.BlockSpec((D, t), lambda h, j: (h, 0))
    kv_in = pl.BlockSpec((bk, D), lambda h, j: (j, 0))
    table = pl.BlockSpec((t, D), lambda h, j: (0, 0), pipeline_mode=pl.Buffered(1))
    return pl.pallas_call(
        functools.partial(bwd_kernel, bq=bq, bk=bk, t=t, nh=nh, n_dev=n_dev),
        grid=(nh, nj),
        in_specs=[col, row_t, col, row_t, col, col, kv_in, kv_in, table, table, hbm, hbm],
        out_specs=[hbm] * 4,
        out_shape=[shape((t, e + 2 * D), bf16), shape((n_dev, rows, e), bf16),
                   shape((n_dev, rows, (nh - 1) * D), bf16),
                   shape((n_dev * e, dwo.shape[1]), bf16)],
        scratch_shapes=[pltpu.VMEM((t, D), f32), pltpu.VMEM((t, D), f32), pltpu.VMEM((D, t), f32), pltpu.VMEM((D, t), f32),
                        pltpu.VMEM((nh, t, D), bf16), pltpu.VMEM((t, D), bf16), pltpu.VMEM((t, D), bf16),
                        dma((1 + nh + 2 * nj,)), dma((n_dev,)), dma((n_dev,)), dma((nh - 1, n_dev)), dma((nh - 1, n_dev)),
                        dma((2,)), dma((7, 2)), dma((7, 2))],
        compiler_params=params(2, collective_id=0),
        name="attn_bwd")(q, qt, do, dot, o, lse, k, v, cos, sin, o, dwo)


N_CHUNK = 6
K_STEP = 4
N_COL = 12
N_ROW = 6


def tail_kernel(h_ref, g_vm, wo_ref, wq_ref, wk_ref, wv_ref, x_ref, lnw_ref, g_own, g_tok, o_tok,
                a_ref, dx_ref, dl_ref, dw_all, g_late,
                gt, acc, stage, lhs, dh, dlw, a2a_send, a2a_recv, ag_send, ag_recv, dl_send, dl_recv, st_sem, lhs_sem,
                *, n_dev):
    step = pl.program_id(0)
    me = lax.axis_index('sp')
    t, width = g_vm.shape
    rows = t // n_dev
    qe = width - 2 * D
    early = g_tok.shape[2]
    late = width - early
    dim = x_ref.shape[1]
    chunk = dim // N_CHUNK
    kk = t // K_STEP
    s_a = N_CHUNK * K_STEP
    s_dh = s_a + N_COL
    s_ln = s_dh + N_COL
    cw = dim // N_COL
    last = s_ln + N_ROW - 1
    peers = [me] + [peer_of(me, rel) for rel in others(n_dev)]

    def rows_of(dev):
        return pl.ds(pl.multiple_of(dev * rows, rows), rows)

    def late_copy(rel):
        return remote(g_own.at[rows_of(peers[rel]), pl.ds(early, late)], g_late.at[me], (a2a_send, a2a_recv), rel, peers[rel])

    def piece(owner, n):
        return dw_all.at[pl.ds(pl.multiple_of(owner * dim + n * chunk, chunk), chunk)]

    def ag_copy(kind, n):
        return gather_copy(kind, n, lambda m: piece(me, m), piece, (ag_send, ag_recv), me)

    def dl_copy(rel):
        return remote(dlw.at[me], dlw.at[me], (dl_send, dl_recv), rel, peers[rel])

    def store_chunk(n):
        return pltpu.make_async_copy(stage.at[n % 2], piece(me, n), st_sem.at[n % 2])

    def o_load(rel):
        src = peers[rel]
        return pltpu.make_async_copy(o_tok.at[src], lhs.at[:, pl.ds(pl.multiple_of(src * qe, D), qe)], lhs_sem.at[0, rel])

    def g_load(rel):
        src = peers[rel]
        if rel == 0:
            first, second, base = g_own.at[rows_of(me), pl.ds(0, early)], g_own.at[rows_of(me)], early
        else:
            first, second, base = g_tok.at[src], g_late.at[src], 0
        n_q = qe - early
        col = pl.multiple_of(src * qe, D)
        kcol = pl.multiple_of(dim + src * D, D)
        vcol = pl.multiple_of(dim + n_dev * D + src * D, D)
        return [pltpu.make_async_copy(first, lhs.at[:, pl.ds(col, early)], lhs_sem.at[1, rel]),
                pltpu.make_async_copy(second.at[:, pl.ds(base, n_q)], lhs.at[:, pl.ds(col + early, n_q)], lhs_sem.at[2, rel]),
                pltpu.make_async_copy(second.at[:, pl.ds(base + n_q, D)], lhs.at[:, pl.ds(kcol, D)], lhs_sem.at[3, rel]),
                pltpu.make_async_copy(second.at[:, pl.ds(base + n_q + D, D)], lhs.at[:, pl.ds(vcol, D)], lhs_sem.at[4, rel])]

    @pl.when(step == 0)
    def _():
        meet_peers(me, n_dev)
        for rel in (6, 7, 2, 4, 3, 5, 1):
            late_copy(rel).start()
        for rel in range(n_dev):
            o_load(rel).start()

        def flip(i, carry):
            r = pl.ds(pl.multiple_of(i * 512, 512), 512)
            gt[:, r] = g_vm[r, :].T
            return carry
        lax.fori_loop(0, t // 512, flip, 0)

    for n in range(N_CHUNK):
        @pl.when(step == (n + 1) * K_STEP)
        def _():
            store_chunk(n).wait()
            for kind in range(3):
                ag_copy(kind, n).start()

    @pl.when(step < s_a)
    def _():
        k = step % K_STEP
        part = jnp.dot(gt[:, pl.ds(pl.multiple_of(k * kk, kk), kk)], h_ref[:], preferred_element_type=f32)

        @pl.when(k == 0)
        def _():
            acc[:] = part

        @pl.when(k > 0)
        def _():
            acc[:] += part

    for n in range(N_CHUNK):
        @pl.when(step == (n + 1) * K_STEP - 1)
        def _():
            stage[n % 2] = acc[:].T.astype(bf16)
            store_chunk(n).start()

    @pl.when(step == s_a)
    def _():
        for rel in range(n_dev):
            o_load(rel).wait()

    @pl.when((step >= s_a) & (step < s_dh))
    def _():
        a_ref[:] = jnp.dot(lhs[:, :dim], wo_ref[:], preferred_element_type=f32).astype(bf16)

    @pl.when(step == s_dh)
    def _():
        for rel in others(n_dev):
            late_copy(rel).wait_recv()
        for rel in range(n_dev):
            for copy in g_load(rel):
                copy.start()
        for rel in range(n_dev):
            for copy in g_load(rel):
                copy.wait()

    for n in range(N_COL):
        @pl.when(step == s_dh + n)
        def _():
            kv = n_dev * D
            dh[:, n * cw:(n + 1) * cw] = (
                lax.dot_general(lhs[:, :dim], wq_ref[:], NT, preferred_element_type=f32)
                + lax.dot_general(lhs[:, dim:dim + kv], wk_ref[:], NT, preferred_element_type=f32)
                + lax.dot_general(lhs[:, dim + kv:], wv_ref[:], NT, preferred_element_type=f32))

    @pl.when(step >= s_ln)
    def _():
        n = step - s_ln
        br = rows // N_ROW
        x = x_ref[:].astype(f32)
        grad = dh[pl.ds(pl.multiple_of(n * br, br), br), :]
        cen = x - jnp.mean(x, axis=1, keepdims=True)
        rstd = lax.rsqrt(jnp.mean(cen * cen, axis=1, keepdims=True) + LN_EPS)
        xhat = cen * rstd
        dy = grad * lnw_ref[:].astype(f32)
        m1 = jnp.mean(dy, axis=1, keepdims=True)
        m2 = jnp.mean(dy * xhat, axis=1, keepdims=True)
        dx_ref[:] = (rstd * (dy - m1 - xhat * m2)).astype(bf16)
        part = jnp.sum((grad * xhat).reshape(br // 8, 8, dim), axis=0)

        @pl.when(n == 0)
        def _():
            dlw[me] = part

        @pl.when(n > 0)
        def _():
            dlw[me] += part

    @pl.when(step == last)
    def _():
        for rel in others(n_dev):
            dl_copy(rel).start()
        for n in range(N_CHUNK):
            ag_copy(0, n).wait_recv()
            if n % 2 == 0:
                ag_copy(3, n).start()
            ag_copy(4, n).start()
            ag_copy(1, n).wait_recv()
            if n % 2 == 1:
                ag_copy(3, n).start()
            ag_copy(5, n).start()
        for n in range(N_CHUNK):
            ag_copy(3, n).wait_recv()
            ag_copy(6, n).start()
        for rel in others(n_dev):
            dl_copy(rel).wait()
            late_copy(rel).wait_send()
        total = dlw[0]
        for dev in others(n_dev):
            total = total + dlw[dev]
        dl_ref[:] = jnp.sum(total, axis=0, keepdims=True).astype(bf16)
        for n in range(N_CHUNK):
            for kind in (2, 4, 5, 6):
                ag_copy(kind, n).wait_recv()
        for n in range(N_CHUNK):
            for kind in range(7):
                ag_copy(kind, n).wait_send()


def tail(h_all, g_own, g_tok, o_tok, w_o, w_q, w_k, w_v, x, lnw, n_dev):
    t, dim = h_all.shape
    width = g_own.shape[1]
    rows = t // n_dev
    s_a = N_CHUNK * K_STEP
    s_dh = s_a + N_COL
    s_ln = s_dh + N_COL
    chunk, cw, br = dim // N_CHUNK, dim // N_COL, rows // N_ROW
    early = g_tok.shape[2]
    kv = w_k.shape[1]

    def h_map(s):
        c = jnp.minimum(s, s_a - 1)
        return c % K_STEP, c // K_STEP

    def at(first, count):
        return lambda s: jnp.clip(s - first, 0, count - 1)

    col_a, col_h, row_l = at(s_a, N_COL), at(s_dh, N_COL), at(s_ln, N_ROW)
    return pl.pallas_call(
        functools.partial(tail_kernel, n_dev=n_dev),
        grid=(s_ln + N_ROW,),
        in_specs=[pl.BlockSpec((t // K_STEP, chunk), h_map),
                  pl.BlockSpec((t, width), fixed, pipeline_mode=pl.Buffered(1)),
                  pl.BlockSpec((dim, cw), lambda s: (0, col_a(s))),
                  pl.BlockSpec((cw, dim), lambda s: (col_h(s), 0)),
                  pl.BlockSpec((cw, kv), lambda s: (col_h(s), 0)),
                  pl.BlockSpec((cw, kv), lambda s: (col_h(s), 0)),
                  pl.BlockSpec((br, dim), lambda s: (row_l(s), 0)),
                  pl.BlockSpec((1, dim), fixed),
                  hbm, hbm, hbm],
        out_specs=[pl.BlockSpec((rows, cw), lambda s: (0, col_a(s))),
                   pl.BlockSpec((br, dim), lambda s: (row_l(s), 0)),
                   pl.BlockSpec((1, dim), fixed),
                   hbm, hbm],
        out_shape=[shape((rows, dim), bf16), shape((rows, dim), bf16),
                   shape((1, dim), bf16), shape((n_dev * dim, width), bf16),
                   shape((n_dev, rows, width - early), bf16)],
        scratch_shapes=[pltpu.VMEM((width, t), bf16), pltpu.VMEM((width, chunk), f32), pltpu.VMEM((2, chunk, width), bf16),
                        pltpu.VMEM((rows, dim + 2 * kv), bf16), pltpu.VMEM((rows, dim), f32), pltpu.VMEM((n_dev, 8, dim), f32),
                        dma((n_dev,)), dma((n_dev,)), dma((7, N_CHUNK)), dma((7, N_CHUNK)),
                        dma((n_dev,)), dma((n_dev,)), dma((2,)), dma((5, n_dev))],
        compiler_params=params(1, collective_id=1),
        name="tail")(h_all, g_own, w_o, w_q, w_k, w_v, x, lnw, g_own, g_tok, o_tok)


def spread_kernel(src_ref, a_ref, dx_ref, wo_ref, q_ref, k_ref, v_ref, a_out, dx_out, wo_out):
    n_dev, _, width = src_ref.shape
    qe = width - 2 * D
    for dev in range(n_dev):
        q_ref[:, dev * qe:(dev + 1) * qe] = src_ref[dev, :, :qe]
        k_ref[:, dev * D:(dev + 1) * D] = src_ref[dev, :, qe:qe + D]
        v_ref[:, dev * D:(dev + 1) * D] = src_ref[dev, :, qe + D:]
    a_out[:] = a_ref[:]
    dx_out[:] = dx_ref[:]
    wo_out[:] = wo_ref[:]


def spread(dw_all, a, dx, dwo, steps=12):
    n_dev, dim, width = dw_all.shape
    bt = dim // steps
    qe = width - 2 * D
    same = [(x, pl.BlockSpec((x.shape[0] // steps, x.shape[1]), rows_at)) for x in (a, dx, dwo)]
    cols = [n_dev * c for c in (qe, D, D)]
    return pl.pallas_call(
        spread_kernel,
        grid=(steps,),
        in_specs=[pl.BlockSpec((n_dev, bt, width), lambda i: (0, i, 0))] + [spec for _, spec in same],
        out_specs=[pl.BlockSpec((bt, c), rows_at) for c in cols] + [spec for _, spec in same],
        out_shape=[shape((dim, c), bf16) for c in cols] + [shape(x.shape, bf16) for x, _ in same],
        compiler_params=params(),
        name="spread")(dw_all, a, dx, dwo)


def solution(mesh):
    n_dev = mesh.shape['sp']
    row_spec = P(('dp', 'sp'), None)
    pos_spec = P(('dp', 'sp'))
    full_spec = P(None, None)
    grad_spec = P('dp', None)

    def local_step(hidden, positions, d_attn, ln_weight, w_q, w_k, w_v, w_o):
        rows, dim = hidden.shape
        qe = w_q.shape[1] // n_dev
        ke = w_k.shape[1] // n_dev
        lane = jnp.arange(D, dtype=jnp.int32)
        freq = ROPE_BASE ** (-(lane - lane % 2).astype(f32) / D)
        pos = jnp.pad(positions.reshape(N_SUB, rows // N_SUB // D, D), ((0, 0), (0, 8 - rows // N_SUB // D), (0, 0)))
        q, qt, k, v, vt, cos, sin, h_all = start(hidden, ln_weight.reshape(1, dim), w_q, w_k, w_v, freq.reshape(1, D), pos, qe // D, n_dev)
        o, ot, lse, g_first = attn_fwd(q, k, vt, d_attn, rows * 2 // 3, n_dev)
        do, dot, dwo_own, _ = mid(g_first, ot, w_o, d_attn, n_dev)
        g_own, o_tok, g_tok, dw_o = attn_bwd(q, qt, do, dot, o, lse, k, v, cos, sin, dwo_own, n_dev)
        attn_out, d_hid, d_lnw, dw_all, _ = tail(h_all, g_own, g_tok, o_tok, w_o, w_q, w_k, w_v, hidden,
                                                 ln_weight.reshape(1, dim), n_dev)
        dw_q, dw_k, dw_v, attn_out, d_hid, dw_o = spread(dw_all.reshape(n_dev, dim, qe + 2 * ke), attn_out, d_hid, dw_o)
        return attn_out, d_hid, d_lnw.reshape(dim), dw_q, dw_k, dw_v, dw_o

    return jax.shard_map(local_step, mesh=mesh,
                         in_specs=(row_spec, pos_spec, row_spec, P(None), full_spec, full_spec, full_spec, full_spec),
                         out_specs=(row_spec, row_spec, P('dp'), grad_spec, grad_spec, grad_spec, grad_spec),
                         check_vma=False)
```

```python
import functools
import math
import jax
import jax.numpy as jnp
from jax import lax
from jax.experimental import pallas as pl
from jax.experimental.pallas import tpu as pltpu
from jax.sharding import PartitionSpec as P

D = 128
LN_EPS = 1e-5
ROPE_BASE = 10000.0
SCALE = D ** -0.5
SCALE2 = SCALE * math.log2(math.e)
NT = (((1,), (1,)), ((), ()))
f32 = jnp.float32
bf16 = jnp.bfloat16
VMEM_LIMIT = 60 * 2 ** 20
shape = jax.ShapeDtypeStruct
dma = pltpu.SemaphoreType.DMA
hbm = pl.BlockSpec(memory_space=pltpu.HBM)


def params(axes=1, **more):
    more.update(has_side_effects=bool(more))
    return pltpu.CompilerParams(vmem_limit_bytes=VMEM_LIMIT, dimension_semantics=("arbitrary",) * axes, **more)


def fixed(i):
    return 0, 0


def rows_at(i):
    return i, 0


def cols_at(i):
    return 0, i


def others(n_dev):
    return range(1, n_dev)


def lanes(h):
    return slice(h * D, (h + 1) * D)


def norm_f32(hid_f32, weight_f32):
    mean_val = jnp.mean(hid_f32, axis=-1, keepdims=True)
    centered = hid_f32 - mean_val
    var_val = jnp.mean(centered * centered, axis=-1, keepdims=True)
    return centered * lax.rsqrt(var_val + LN_EPS) * weight_f32


SIB, XN, YN, DIAG = 1, 2, 4, 6


def peer_of(me, rel):
    mine = (me % 2, (me // 2) % 2, me // 4)
    flip = (rel % 2, (rel // 2) % 2, rel // 4)
    return sum(((mine[n] + flip[n]) % 2) * (1 << n) for n in range(3))


def remote(src, dst, sems, slot, target):
    return pltpu.make_async_remote_copy(
        src_ref=src, dst_ref=dst, send_sem=sems[0].at[slot], recv_sem=sems[1].at[slot],
        device_id={'sp': target}, device_id_type=pl.DeviceIdType.MESH)


def meet_peers(me, n_dev):
    barrier = pltpu.get_barrier_semaphore()
    for rel in others(n_dev):
        pl.semaphore_signal(barrier, device_id={'sp': peer_of(me, rel)}, device_id_type=pl.DeviceIdType.MESH)
    pl.semaphore_wait(barrier, n_dev - 1)


def gather_copy(kind, n, own, piece, sems, me):
    if kind == 3:
        owner, target = (XN, YN) if n % 2 == 0 else (YN, XN)
    else:
        owner, target = {0: (0, XN), 1: (0, YN), 2: (0, SIB), 4: (XN, SIB), 5: (YN, SIB), 6: (DIAG, SIB)}[kind]
    dst = piece(peer_of(me, owner), n)
    return remote(own(n) if owner == 0 else dst, dst, (sems[0].at[kind], sems[1].at[kind]), n, peer_of(me, target))


def rotate(val, cos, sin):
    even = lax.rem(lax.broadcasted_iota(jnp.int32, val.shape, 1), 2) == 0
    swapped = jnp.where(even, pltpu.roll(val, D - 1, 1), pltpu.roll(val, 1, 1))
    return val * cos + swapped * sin


N_SUB = 3


def item_of(s, n_dev):
    n_mid = 4 * N_SUB
    first = 2 * N_SUB
    u, w = s - first, s - first - n_mid
    r = u % 4
    rel = jnp.where(s < first, s // N_SUB, jnp.where(s < first + n_mid, 2 + 2 * (r % 2) + r // 2, 6 + w % 2))
    m = jnp.where(s < first, s % N_SUB, jnp.where(s < first + n_mid, u // 4, w // 2))
    return rel, m


def items(n_dev):
    out = [(rel, m) for rel in (0, SIB) for m in range(N_SUB)]
    out += [(rel, m) for m in range(N_SUB) for rel in (XN, YN, XN + 1, YN + 1)]
    return out + [(rel, m) for m in range(N_SUB) for rel in (DIAG, DIAG + 1)]


def start_kernel(x_ref, lnw_ref, wq_hbm, wk_hbm, wv_hbm, freq_ref, pos_ref, q_ref, qt_ref, k_ref, v_ref, vt_ref, cos_ref, sin_ref, h_all,
                 w_ref, hs, buf, pos_all, w_sem, loc_sem, ld_sem, pos_send, pos_recv, ag_send, ag_recv, *, n_dev, nh):
    step = pl.program_id(0)
    me = lax.axis_index('sp')
    rows = x_ref.shape[0]
    size = rows // (2 * N_SUB)
    sub = 2 * size
    order = items(n_dev)
    rel_t, m_t = item_of(step, n_dev)
    owner_t = peer_of(me, rel_t)

    def own(n):
        return hs.at[pl.ds(pl.multiple_of(n * size, size), size)]

    def piece(owner, n):
        return h_all.at[pl.ds(pl.multiple_of(owner * rows + n * size, size), size)]

    def copy(kind, n):
        return gather_copy(kind, n, own, piece, (ag_send, ag_recv), me)

    def pos_copy(rel):
        return remote(pos_all.at[me], pos_all.at[me], (pos_send, pos_recv), rel, peer_of(me, rel))

    def keep_own():
        return pltpu.make_async_copy(hs, h_all.at[pl.ds(pl.multiple_of(me * rows, rows), rows)], loc_sem)

    def load(i):
        rel, m = order[i]
        src = h_all.at[pl.ds(pl.multiple_of(peer_of(me, rel) * rows + m * sub, sub), sub)]
        return pltpu.make_async_copy(src, buf.at[i % 2], ld_sem.at[i % 2])

    def arrive(i):
        rel, m = order[i]
        for n in (2 * m, 2 * m + 1):
            if rel == SIB:
                copy(2, n).wait_recv()
            elif rel in (XN, YN):
                copy(0 if rel == XN else 1, n).wait_recv()
                if (rel == XN) == (n % 2 == 0):
                    copy(3, n).start()
                copy(4 if rel == XN else 5, n).start()
            elif rel in (XN + 1, YN + 1):
                copy(4 if rel == XN + 1 else 5, n).wait_recv()
            elif rel == DIAG:
                copy(3, n).wait_recv()
                copy(6, n).start()
            elif rel == DIAG + 1:
                copy(6, n).wait_recv()

    def w_load(i):
        col, size_w, src = ((0, nh * D, wq_hbm), (nh * D, D, wk_hbm), ((nh + 1) * D, D, wv_hbm))[i]
        return pltpu.make_async_copy(src.at[:, pl.ds(pl.multiple_of(me * size_w, D), size_w)], w_ref.at[:, pl.ds(col, size_w)], w_sem.at[i])

    @pl.when(step == 0)
    def _():
        for i in range(3):
            w_load(i).start()
        pos_all[me] = pos_ref[:]
        meet_peers(me, n_dev)

        def norm(n, carry):
            r = pl.ds(pl.multiple_of(n * size, size), size)
            hs[r, :] = norm_f32(x_ref[r, :].astype(f32), lnw_ref[:].astype(f32)).astype(bf16)

            @pl.when(n > 0)
            def _():
                for kind in range(3):
                    copy(kind, n - 1).start()
            return carry
        lax.fori_loop(0, 2 * N_SUB, norm, 0)
        for rel in others(n_dev):
            pos_copy(rel).start()
        for kind in range(3):
            copy(kind, 2 * N_SUB - 1).start()
        keep_own().start()
        keep_own().wait()
        load(0).start()
        for i in range(3):
            w_load(i).wait()

    for i in range(1, len(order)):
        @pl.when(step == i - 1)
        def _():
            if i == N_SUB:
                for rel in others(n_dev):
                    pos_copy(rel).wait_recv()
            arrive(i)
            load(i).start()

    slot = step % 2
    pltpu.make_async_copy(h_all.at[pl.ds(0, sub)], buf.at[slot], ld_sem.at[slot]).wait()
    tile = pos_all[owner_t, m_t].astype(f32)
    pos = jnp.concatenate([jnp.broadcast_to(tile[i:i + 1, :], (D, D)).T for i in range(sub // D)], axis=0)
    angles = pos * freq_ref[:]
    cos = jnp.cos(angles)
    sin = jnp.sin(angles)
    sin = jnp.where(lax.rem(lax.broadcasted_iota(jnp.int32, sin.shape, 1), 2) == 0, -sin, sin)
    cos_ref[:] = cos
    sin_ref[:] = sin
    res = jnp.dot(buf[slot], w_ref[:], preferred_element_type=f32)
    for n in range(nh):
        rot = rotate(res[:, lanes(n)], cos, sin).astype(bf16)
        q_ref[:, lanes(n)] = rot
        qt_ref[lanes(n), :] = rot.T
    k_ref[:] = rotate(res[:, lanes(nh)], cos, sin).astype(bf16)
    v = res[:, (nh + 1) * D:].astype(bf16)
    v_ref[:] = v
    vt_ref[:] = v.T

    @pl.when(step == len(order) - 1)
    def _():
        for rel in others(n_dev):
            pos_copy(rel).wait_send()
        for n in range(2 * N_SUB):
            for kind in range(7):
                copy(kind, n).wait_send()


def start(x, lnw, w_q, w_k, w_v, freq, pos, nh, n_dev):
    rows, dim = x.shape
    t = rows * n_dev
    sub = rows // N_SUB
    whole = lambda a: pl.BlockSpec(a.shape, lambda s: (0,) * a.ndim, pipeline_mode=pl.Buffered(1))

    def at(s):
        rel, m = item_of(s, n_dev)
        return peer_of(lax.axis_index('sp'), rel) * N_SUB + m

    row = lambda c: pl.BlockSpec((sub, c), lambda s: (at(s), 0))
    col = lambda r: pl.BlockSpec((r, sub), lambda s: (0, at(s)))
    return pl.pallas_call(
        functools.partial(start_kernel, n_dev=n_dev, nh=nh),
        grid=(n_dev * N_SUB,),
        in_specs=[whole(x), whole(lnw), hbm, hbm, hbm, whole(freq), whole(pos)],
        out_specs=[row(nh * D), col(nh * D), row(D), row(D), col(D), row(D), row(D), hbm],
        out_shape=[shape((t, nh * D), bf16), shape((nh * D, t), bf16), shape((t, D), bf16), shape((t, D), bf16), shape((D, t), bf16),
                   shape((t, D), f32), shape((t, D), f32), shape((t, dim), bf16)],
        scratch_shapes=[pltpu.VMEM((dim, (nh + 2) * D), bf16), pltpu.VMEM((rows, dim), bf16), pltpu.VMEM((2, sub, dim), bf16),
                        pltpu.VMEM((n_dev,) + pos.shape, jnp.int32), dma((3,)), dma, dma((2,)), dma((n_dev,)), dma((n_dev,)), dma((7, 2 * N_SUB)), dma((7, 2 * N_SUB))],
        compiler_params=params(1, collective_id=4),
        name="start")(x, lnw, w_q, w_k, w_v, freq, pos)


def mid_kernel(g_blk, ot_hbm, w_hbm, g_own, do_ref, dot_ref, dwo_ref, g_rest, ot_ref, w_ref, op_sem, acc, buf, ld_sem, ag_send, ag_recv, *, n_dev, rows, first):
    step = pl.program_id(0)
    me = lax.axis_index('sp')
    rest = rows - first
    half = rest // 2
    order = (0, SIB, XN, YN, XN + 1, YN + 1, DIAG, DIAG + 1)

    def own(n):
        return g_own.at[pl.ds(first + n * half, half)]

    def piece(owner, n):
        return g_rest.at[pl.ds(pl.multiple_of(owner * rest + n * half, half), half)]

    def copy(kind, n):
        return gather_copy(kind, n, own, piece, (ag_send, ag_recv), me)

    def load(i):
        owner = peer_of(me, order[i])
        src = g_own.at[pl.ds(first, rest)] if i == 0 else g_rest.at[pl.ds(pl.multiple_of(owner * rest, rest), rest)]
        return pltpu.make_async_copy(src, buf.at[i % 2], ld_sem.at[i % 2])

    def compute(g, row0, size):
        r = pl.ds(row0, size)
        val = lax.dot_general(g, w_ref[:], NT, preferred_element_type=f32).astype(bf16)
        do_ref[r, :] = val
        dot_ref[:, r] = val.T
        acc[:] += jnp.dot(ot_ref[:, r], g, preferred_element_type=f32)

    @pl.when(step == 0)
    def _():
        meet_peers(me, n_dev)
        for n in range(2):
            for kind in range(3):
                copy(kind, n).start()
        e = w_ref.shape[0]
        fetch = [pltpu.make_async_copy(ot_hbm, ot_ref, op_sem.at[0]),
                 pltpu.make_async_copy(w_hbm.at[pl.ds(pl.multiple_of(me * e, D), e)], w_ref, op_sem.at[1])]
        for copy_in in fetch:
            copy_in.start()
        acc[:] = jnp.zeros_like(acc)
        for copy_in in fetch:
            copy_in.wait()

    @pl.when(step == 5)
    def _():
        copy(0, 0).wait_recv()
        copy(3, 0).start()
        copy(4, 0).start()

    @pl.when(step == n_dev)
    def _():
        copy(1, 1).wait_recv()
        copy(3, 1).start()
        copy(5, 1).start()
        copy(0, 1).wait_recv()
        copy(4, 1).start()
        copy(1, 0).wait_recv()
        copy(5, 0).start()

    waits = {1: ((2, 0), (2, 1)), 4: ((4, 0), (4, 1)), 5: ((5, 0), (5, 1)), 6: ((3, 0), (3, 1)), 7: ((6, 0), (6, 1))}
    for i in range(n_dev):
        @pl.when(step == n_dev - 1 + i)
        def _():
            for kind, n in waits.get(i, ()):
                copy(kind, n).wait_recv()
                if kind == 3:
                    copy(6, n).start()
            load(i).start()

    @pl.when(step < n_dev)
    def _():
        compute(g_blk[:], pl.multiple_of(step * rows, D), first)

    @pl.when(step >= n_dev)
    def _():
        i = step - n_dev
        u = i - XN
        rel = jnp.where((u >= 0) & (u < 4), XN + 2 * (u % 2) + u // 2, i)
        slot = i % 2
        pltpu.make_async_copy(g_own.at[pl.ds(first, rest)], buf.at[slot], ld_sem.at[slot]).wait()
        compute(buf[slot], pl.multiple_of(peer_of(me, rel) * rows + first, D), rest)

    @pl.when(step == 2 * n_dev - 1)
    def _():
        dwo_ref[:] = acc[:].astype(bf16)
        for n in range(2):
            for kind in range(7):
                copy(kind, n).wait_send()


def mid(g_first, ot, w, g_own, n_dev):
    dim = g_own.shape[1]
    rows = g_own.shape[0]
    first = g_first.shape[0] // n_dev
    rest = rows - first
    e, t = ot.shape
    const = lambda a, b: pl.BlockSpec((a, b), fixed)
    return pl.pallas_call(
        functools.partial(mid_kernel, n_dev=n_dev, rows=rows, first=first),
        grid=(2 * n_dev,),
        in_specs=[pl.BlockSpec((first, dim), lambda i: (jnp.minimum(i, n_dev - 1), 0)), hbm, hbm, hbm],
        out_specs=[const(t, e), const(e, t), const(e, dim), hbm],
        out_shape=[shape((t, e), bf16), shape((e, t), bf16), shape((e, dim), bf16),
                   shape((n_dev * rest, dim), bf16)],
        scratch_shapes=[pltpu.VMEM((e, t), bf16), pltpu.VMEM((e, dim), bf16), dma((2,)),
                        pltpu.VMEM((e, dim), f32), pltpu.VMEM((2, rest, dim), bf16), dma((2,)), dma((7, 2)), dma((7, 2))],
        compiler_params=params(1, collective_id=3),
        name="mid")(g_first, ot, w, g_own)


def fwd_kernel(q_ref, k_ref, vt_ref, g_own, o_ref, ot_ref, lse_ref, g_first, acc, m_ref, l_ref, loc_sem, ag_send, ag_recv,
               *, bq, bk, nh, n_dev, first, n_piece):
    i = pl.program_id(0)
    nq = pl.num_programs(0)
    me = lax.axis_index('sp')
    size = first // n_piece

    def own(n):
        return g_own.at[pl.ds(n * size, size)]

    def piece(owner, n):
        return g_first.at[pl.ds(pl.multiple_of(owner * first + n * size, size), size)]

    def copy(kind, n):
        return gather_copy(kind, n, own, piece, (ag_send, ag_recv), me)

    def keep_own():
        return pltpu.make_async_copy(g_own.at[pl.ds(0, first)], g_first.at[pl.ds(pl.multiple_of(me * first, first), first)], loc_sem)

    def pass_on(n):
        copy(0, n).wait_recv()
        copy(1, n).wait_recv()
        copy(3, n).start()
        copy(4, n).start()
        copy(5, n).start()

    @pl.when(i == 0)
    def _():
        meet_peers(me, n_dev)
        for n in range(n_piece):
            for kind in range(3):
                copy(kind, n).start()
        keep_own().start()

    @pl.when(i == nq - 2)
    def _():
        for n in range(n_piece // 2):
            pass_on(n)

    @pl.when(i == nq - 1)
    def _():
        for n in range(n_piece // 2, n_piece):
            pass_on(n)

    for h in range(nh):
        m_ref[h:h + 1, :] = jnp.full((1, bq), -1e30, f32)
        l_ref[h:h + 1, :] = jnp.zeros((1, bq), f32)
    acc[:] = jnp.zeros_like(acc)

    def step(off, diag):
        q0 = 0 if diag is None else diag
        kb = k_ref[pl.ds(off, bk), :]
        vt = vt_ref[:, pl.ds(off, bk)]
        if diag is not None:
            ki = lax.broadcasted_iota(jnp.int32, (bk, bq - q0), 0)
            qi = lax.broadcasted_iota(jnp.int32, (bk, bq - q0), 1)
            keep = ki <= qi
        ss = [lax.dot_general(kb, q_ref[q0:, lanes(h)], NT, preferred_element_type=f32) for h in range(nh)]
        for h in range(nh):
            s = ss[h]
            if diag is not None:
                s = jnp.where(keep, s, -1e30)
            m_old = m_ref[h:h + 1, q0:]
            m_new = jnp.maximum(m_old, jnp.max(s, axis=0, keepdims=True))
            p = jnp.exp2(s * SCALE2 - m_new * SCALE2)
            alpha = jnp.exp2((m_old - m_new) * SCALE2)
            m_ref[h:h + 1, q0:] = m_new
            l_ref[h:h + 1, q0:] = l_ref[h:h + 1, q0:] * alpha + jnp.sum(p, axis=0, keepdims=True)
            pv = jnp.dot(vt, p.astype(bf16), preferred_element_type=f32)
            acc[lanes(h), q0:] = acc[lanes(h), q0:] * alpha + pv

    ratio = bq // bk

    def body(j, carry):
        step(pl.multiple_of(j * bk, bk), None)
        return carry

    lax.fori_loop(0, i * ratio, body, 0)
    for d in range(ratio):
        step(pl.multiple_of(i * bq + d * bk, bk), d * bk)
    for h in range(nh):
        m = m_ref[h:h + 1, :]
        l = l_ref[h:h + 1, :]
        out_t = acc[lanes(h), :] * (1.0 / l)
        o_ref[:, lanes(h)] = out_t.T.astype(bf16)
        ot_ref[lanes(h), :] = out_t.astype(bf16)
        lse_ref[:, lanes(h)] = jnp.broadcast_to(m * SCALE2 + jnp.log2(l), (D, bq)).T

    @pl.when(i == nq - 1)
    def _():
        for n in range(n_piece):
            copy(3, n).wait_recv()
            copy(6, n).start()
        keep_own().wait()
        for n in range(n_piece):
            for kind in (2, 4, 5, 6):
                copy(kind, n).wait_recv()
            for kind in range(7):
                copy(kind, n).wait_send()


def attn_fwd(q, k, vt, g_own, first, n_dev, bq=1024, bk=512, n_piece=4):
    t, e = q.shape
    nh = e // D
    row = pl.BlockSpec((bq, e), rows_at)
    return pl.pallas_call(
        functools.partial(fwd_kernel, bq=bq, bk=bk, nh=nh, n_dev=n_dev, first=first, n_piece=n_piece),
        grid=(t // bq,),
        in_specs=[row, pl.BlockSpec((t, D), fixed), pl.BlockSpec((D, t), fixed), hbm],
        out_specs=[row, pl.BlockSpec((e, bq), cols_at), row, hbm],
        out_shape=[shape((t, e), bf16), shape((e, t), bf16), shape((t, e), f32),
                   shape((n_dev * first, g_own.shape[1]), bf16)],
        scratch_shapes=[pltpu.VMEM((e, bq), f32), pltpu.VMEM((8, bq), f32), pltpu.VMEM((8, bq), f32), dma, dma((7, n_piece)), dma((7, n_piece))],
        compiler_params=params(1, collective_id=2),
        name="attn_fwd")(q, k, vt, g_own)


def bwd_kernel(q_ref, qt_ref, do_ref, dot_ref, o_ref, lse_ref, k_ref, v_ref, cos_ref, sin_ref, o_all, dwo_own,
               g_own, o_tok, g_tok, dwo_all, dlt, dqa, dka, dva, gqs, gks, gvs, loc_sem, o_send, o_recv, g_send, g_recv,
               w_sem, ag_send, ag_recv, *, bq, bk, t, nh, n_dev):
    h = pl.program_id(0)
    j = pl.program_id(1)
    nj = t // bk
    nq = t // bq
    rep = bk // D
    rows = t // n_dev
    early = nh - 1
    koff = pl.multiple_of(j * bk, bk)
    kc = pl.ds(koff, bk)
    me = lax.axis_index('sp')

    def rows_of(dev):
        return pl.ds(pl.multiple_of(dev * rows, rows), rows)

    def o_copy(rel):
        peer = peer_of(me, rel)
        return remote(o_all.at[rows_of(peer)], o_tok.at[me], (o_send, o_recv), rel, peer)

    def g_copy(head, rel):
        peer = peer_of(me, rel)
        return remote(gqs.at[head, rows_of(peer)], g_tok.at[me, :, pl.ds(head * D, D)],
                      (g_send.at[head], g_recv.at[head]), rel, peer)

    half = dwo_own.shape[0] // 2

    def own(n):
        return dwo_own.at[pl.ds(n * half, half)]

    def piece(owner, n):
        return dwo_all.at[pl.ds(pl.multiple_of((2 * owner + n) * half, half), half)]

    def w_copy(kind, n):
        return gather_copy(kind, n, own, piece, (ag_send, ag_recv), me)

    def w_local(n):
        return pltpu.make_async_copy(own(n), piece(me, n), w_sem.at[n])

    def o_local():
        return pltpu.make_async_copy(o_all.at[rows_of(me)], o_tok.at[me], loc_sem.at[0])

    def gq_local(head):
        return pltpu.make_async_copy(gqs.at[head], g_own.at[:, pl.ds(head * D, D)], loc_sem.at[1 + head])

    def gk_local(jj):
        r = pl.ds(jj * bk, bk)
        return pltpu.make_async_copy(gks.at[r], g_own.at[r, pl.ds(nh * D, D)], loc_sem.at[1 + nh + jj])

    def gv_local(jj):
        r = pl.ds(jj * bk, bk)
        return pltpu.make_async_copy(gvs.at[r], g_own.at[r, pl.ds((nh + 1) * D, D)], loc_sem.at[1 + nh + nj + jj])

    @pl.when((h == 0) & (j == 0))
    def _():
        meet_peers(me, n_dev)
        for rel in others(n_dev):
            o_copy(rel).start()
        o_local().start()
        for n in range(2):
            w_local(n).start()
            for kind in range(3):
                w_copy(kind, n).start()

    @pl.when((h == nh - 1) & (j == 0))
    def _():
        for n in range(2):
            w_copy(0, n).wait_recv()
            w_copy(1, n).wait_recv()
            for kind in (3, 4, 5):
                w_copy(kind, n).start()

    @pl.when(j == 0)
    def _():
        def init(i, carry):
            r = pl.ds(pl.multiple_of(i * bq, bq), bq)
            d = jnp.sum(do_ref[r, :].astype(f32) * o_ref[r, :].astype(f32), axis=1, keepdims=True)
            dlt[r, :] = jnp.broadcast_to(d, (bq, D))
            dqa[r, :] = jnp.zeros((bq, D), f32)
            return carry
        lax.fori_loop(0, nq, init, 0)

    @pl.when(h == 0)
    def _():
        dka[:, kc] = jnp.zeros((D, bk), f32)
        dva[:, kc] = jnp.zeros((D, bk), f32)

    def step(i, diag):
        off = pl.multiple_of(i * bq, bq)
        r = pl.ds(off, bq)
        nk = bk if diag is None else diag + bq
        rep = nk // D
        kc = pl.ds(koff, nk)
        kb, vb = k_ref[:nk, :], v_ref[:nk, :]
        s = lax.dot_general(q_ref[r, :], kb, NT, preferred_element_type=f32)
        dp = lax.dot_general(do_ref[r, :], vb, NT, preferred_element_type=f32)
        if diag is not None:
            qi = lax.broadcasted_iota(jnp.int32, (bq, nk), 0) + diag
            ki = lax.broadcasted_iota(jnp.int32, (bq, nk), 1)
            s = jnp.where(ki <= qi, s, -1e30)
        p = jnp.exp2(s * SCALE2 - jnp.concatenate([lse_ref[r, :]] * rep, axis=1))
        ds = ((dp - jnp.concatenate([dlt[r, :]] * rep, axis=1)) * p * SCALE).astype(bf16)
        dva[:, kc] += jnp.dot(dot_ref[:, r], p.astype(bf16), preferred_element_type=f32)
        dka[:, kc] += jnp.dot(qt_ref[:, r], ds, preferred_element_type=f32)
        dqa[r, :] += jnp.dot(ds, kb, preferred_element_type=f32)

    ratio = max(bk // bq, 1)
    first = (j * bk) // bq
    for d in range(ratio):
        step(first + d, d * bq)

    def body(i, carry):
        step(i, None)
        return carry

    lax.fori_loop(first + ratio, nq, body, 0)

    for head in range(nh):
        @pl.when((j == nj - 1) & (h == head))
        def _():
            def fin(i, carry):
                r = pl.ds(pl.multiple_of(i * bq, bq), bq)
                dq = dqa[r, :].astype(bf16).astype(f32)
                gqs[head, r, :] = rotate(dq, cos_ref[r, :], -sin_ref[r, :]).astype(bf16)
                return carry
            lax.fori_loop(0, nq, fin, 0)
            gq_local(head).start()
            if head < early:
                for rel in others(n_dev):
                    g_copy(head, rel).start()

    for jj in range(nj):
        @pl.when((h == nh - 1) & (j == jj))
        def _():
            dk = dka[:, jj * bk:(jj + 1) * bk].T.astype(bf16).astype(f32)
            r = slice(jj * bk, (jj + 1) * bk)
            gks[r, :] = rotate(dk, cos_ref[r, :], -sin_ref[r, :]).astype(bf16)
            gvs[r, :] = dva[:, jj * bk:(jj + 1) * bk].T.astype(bf16)
            gk_local(jj).start()
            gv_local(jj).start()

    @pl.when((h == nh - 1) & (j == nj - 1))
    def _():
        for n in range(2):
            w_local(n).wait()
            w_copy(3, n).wait_recv()
            w_copy(6, n).start()
        o_local().wait()
        for head in range(nh):
            gq_local(head).wait()
        for jj in range(nj):
            gk_local(jj).wait()
            gv_local(jj).wait()
        for rel in others(n_dev):
            o_copy(rel).wait()
            for head in range(early):
                g_copy(head, rel).wait()
        for n in range(2):
            for kind in (2, 4, 5, 6):
                w_copy(kind, n).wait_recv()
            for kind in range(7):
                w_copy(kind, n).wait_send()


def attn_bwd(q, qt, do, dot, o, lse, k, v, cos, sin, dwo, n_dev, bq=512, bk=1024):
    t, e = q.shape
    nh = e // D
    nj = t // bk
    rows = t // n_dev
    col = pl.BlockSpec((t, D), lambda h, j: (0, h))
    row_t = pl.BlockSpec((D, t), lambda h, j: (h, 0))
    kv_in = pl.BlockSpec((bk, D), lambda h, j: (j, 0))
    table = pl.BlockSpec((t, D), lambda h, j: (0, 0), pipeline_mode=pl.Buffered(1))
    return pl.pallas_call(
        functools.partial(bwd_kernel, bq=bq, bk=bk, t=t, nh=nh, n_dev=n_dev),
        grid=(nh, nj),
        in_specs=[col, row_t, col, row_t, col, col, kv_in, kv_in, table, table, hbm, hbm],
        out_specs=[hbm] * 4,
        out_shape=[shape((t, e + 2 * D), bf16), shape((n_dev, rows, e), bf16),
                   shape((n_dev, rows, (nh - 1) * D), bf16),
                   shape((n_dev * e, dwo.shape[1]), bf16)],
        scratch_shapes=[pltpu.VMEM((t, D), f32), pltpu.VMEM((t, D), f32), pltpu.VMEM((D, t), f32), pltpu.VMEM((D, t), f32),
                        pltpu.VMEM((nh, t, D), bf16), pltpu.VMEM((t, D), bf16), pltpu.VMEM((t, D), bf16),
                        dma((1 + nh + 2 * nj,)), dma((n_dev,)), dma((n_dev,)), dma((nh - 1, n_dev)), dma((nh - 1, n_dev)),
                        dma((2,)), dma((7, 2)), dma((7, 2))],
        compiler_params=params(2, collective_id=0),
        name="attn_bwd")(q, qt, do, dot, o, lse, k, v, cos, sin, o, dwo)


N_CHUNK = 6
K_STEP = 4
N_COL = 12
N_ROW = 6


def tail_kernel(h_ref, wo_ref, wq_ref, wk_ref, wv_ref, x_ref, lnw_ref, g_own, g_tok, o_tok,
                a_ref, dx_ref, dl_ref, dw_all, g_late,
                g_vm, g_sem, gt, acc, stage, lhs, dh, dlw, a2a_send, a2a_recv, ag_send, ag_recv, dl_send, dl_recv, st_sem, lhs_sem,
                *, n_dev):
    step = pl.program_id(0)
    me = lax.axis_index('sp')
    t, width = g_vm.shape
    rows = t // n_dev
    qe = width - 2 * D
    early = g_tok.shape[2]
    late = width - early
    dim = x_ref.shape[1]
    chunk = dim // N_CHUNK
    kk = t // K_STEP
    s_a = N_CHUNK * K_STEP
    s_dh = s_a + N_COL
    s_ln = s_dh + N_COL
    cw = dim // N_COL
    last = s_ln + N_ROW - 1
    peers = [me] + [peer_of(me, rel) for rel in others(n_dev)]

    def rows_of(dev):
        return pl.ds(pl.multiple_of(dev * rows, rows), rows)

    def late_copy(rel):
        return remote(g_own.at[rows_of(peers[rel]), pl.ds(early, late)], g_late.at[me], (a2a_send, a2a_recv), rel, peers[rel])

    def piece(owner, n):
        return dw_all.at[pl.ds(pl.multiple_of(owner * dim + n * chunk, chunk), chunk)]

    def ag_copy(kind, n):
        return gather_copy(kind, n, lambda m: piece(me, m), piece, (ag_send, ag_recv), me)

    def dl_copy(rel):
        return remote(dlw.at[me], dlw.at[me], (dl_send, dl_recv), rel, peers[rel])

    def store_chunk(n):
        return pltpu.make_async_copy(stage.at[n % 2], piece(me, n), st_sem.at[n % 2])

    def o_load(rel):
        src = peers[rel]
        return pltpu.make_async_copy(o_tok.at[src], lhs.at[:, pl.ds(pl.multiple_of(src * qe, D), qe)], lhs_sem.at[0, rel])

    def g_load(rel):
        src = peers[rel]
        if rel == 0:
            first, second, base = g_own.at[rows_of(me), pl.ds(0, early)], g_own.at[rows_of(me)], early
        else:
            first, second, base = g_tok.at[src], g_late.at[src], 0
        n_q = qe - early
        col = pl.multiple_of(src * qe, D)
        kcol = pl.multiple_of(dim + src * D, D)
        vcol = pl.multiple_of(dim + n_dev * D + src * D, D)
        return [pltpu.make_async_copy(first, lhs.at[:, pl.ds(col, early)], lhs_sem.at[1, rel]),
                pltpu.make_async_copy(second.at[:, pl.ds(base, n_q)], lhs.at[:, pl.ds(col + early, n_q)], lhs_sem.at[2, rel]),
                pltpu.make_async_copy(second.at[:, pl.ds(base + n_q, D)], lhs.at[:, pl.ds(kcol, D)], lhs_sem.at[3, rel]),
                pltpu.make_async_copy(second.at[:, pl.ds(base + n_q + D, D)], lhs.at[:, pl.ds(vcol, D)], lhs_sem.at[4, rel])]

    @pl.when(step == 0)
    def _():
        meet_peers(me, n_dev)
        for rel in (6, 7, 2, 4, 3, 5, 1):
            late_copy(rel).start()
        for rel in range(n_dev):
            o_load(rel).start()
        fetch = pltpu.make_async_copy(g_own, g_vm, g_sem)
        fetch.start()
        fetch.wait()

        def flip(i, carry):
            r = pl.ds(pl.multiple_of(i * 512, 512), 512)
            gt[:, r] = g_vm[r, :].T
            return carry
        lax.fori_loop(0, t // 512, flip, 0)

    for n in range(N_CHUNK):
        @pl.when(step == (n + 1) * K_STEP)
        def _():
            store_chunk(n).wait()
            for kind in range(3):
                ag_copy(kind, n).start()

    @pl.when(step < s_a)
    def _():
        k = step % K_STEP
        part = jnp.dot(gt[:, pl.ds(pl.multiple_of(k * kk, kk), kk)], h_ref[:], preferred_element_type=f32)

        @pl.when(k == 0)
        def _():
            acc[:] = part

        @pl.when(k > 0)
        def _():
            acc[:] += part

    @pl.when((step < s_a) & (step % K_STEP == K_STEP - 1))
    def _():
        n = step // K_STEP
        stage[n % 2] = acc[:].T.astype(bf16)
        store_chunk(n).start()

    @pl.when(step == s_a)
    def _():
        for rel in range(n_dev):
            o_load(rel).wait()

    @pl.when((step >= s_a) & (step < s_dh))
    def _():
        a_ref[:] = jnp.dot(lhs[:, :dim], wo_ref[:], preferred_element_type=f32).astype(bf16)

    @pl.when(step == s_dh)
    def _():
        for rel in others(n_dev):
            late_copy(rel).wait_recv()
        for rel in range(n_dev):
            for copy in g_load(rel):
                copy.start()
        for rel in range(n_dev):
            for copy in g_load(rel):
                copy.wait()

    @pl.when((step >= s_dh) & (step < s_ln))
    def _():
        kv = n_dev * D
        dh[:, pl.ds(pl.multiple_of((step - s_dh) * cw, cw), cw)] = (
            lax.dot_general(lhs[:, :dim], wq_ref[:], NT, preferred_element_type=f32)
            + lax.dot_general(lhs[:, dim:dim + kv], wk_ref[:], NT, preferred_element_type=f32)
            + lax.dot_general(lhs[:, dim + kv:], wv_ref[:], NT, preferred_element_type=f32))

    @pl.when(step >= s_ln)
    def _():
        n = step - s_ln
        br = rows // N_ROW
        x = x_ref[:].astype(f32)
        grad = dh[pl.ds(pl.multiple_of(n * br, br), br), :]
        cen = x - jnp.mean(x, axis=1, keepdims=True)
        rstd = lax.rsqrt(jnp.mean(cen * cen, axis=1, keepdims=True) + LN_EPS)
        xhat = cen * rstd
        dy = grad * lnw_ref[:].astype(f32)
        m1 = jnp.mean(dy, axis=1, keepdims=True)
        m2 = jnp.mean(dy * xhat, axis=1, keepdims=True)
        dx_ref[:] = (rstd * (dy - m1 - xhat * m2)).astype(bf16)
        part = jnp.sum((grad * xhat).reshape(br // 8, 8, dim), axis=0)

        @pl.when(n == 0)
        def _():
            dlw[me] = part

        @pl.when(n > 0)
        def _():
            dlw[me] += part

    @pl.when(step == last)
    def _():
        for rel in others(n_dev):
            dl_copy(rel).start()
        for n in range(N_CHUNK):
            ag_copy(0, n).wait_recv()
            if n % 2 == 0:
                ag_copy(3, n).start()
            ag_copy(4, n).start()
            ag_copy(1, n).wait_recv()
            if n % 2 == 1:
                ag_copy(3, n).start()
            ag_copy(5, n).start()
        for n in range(N_CHUNK):
            ag_copy(3, n).wait_recv()
            ag_copy(6, n).start()
        for rel in others(n_dev):
            dl_copy(rel).wait()
            late_copy(rel).wait_send()
        total = dlw[0]
        for dev in others(n_dev):
            total = total + dlw[dev]
        dl_ref[:] = jnp.sum(total, axis=0, keepdims=True).astype(bf16)
        for n in range(N_CHUNK):
            for kind in (2, 4, 5, 6):
                ag_copy(kind, n).wait_recv()
        for n in range(N_CHUNK):
            for kind in range(7):
                ag_copy(kind, n).wait_send()


def tail(h_all, g_own, g_tok, o_tok, w_o, w_q, w_k, w_v, x, lnw, n_dev):
    t, dim = h_all.shape
    width = g_own.shape[1]
    rows = t // n_dev
    s_a = N_CHUNK * K_STEP
    s_dh = s_a + N_COL
    s_ln = s_dh + N_COL
    chunk, cw, br = dim // N_CHUNK, dim // N_COL, rows // N_ROW
    early = g_tok.shape[2]
    kv = w_k.shape[1]

    def h_map(s):
        c = jnp.minimum(s, s_a - 1)
        return c % K_STEP, c // K_STEP

    def at(first, count):
        return lambda s: jnp.clip(s - first, 0, count - 1)

    col_a, col_h, row_l = at(s_a, N_COL), at(s_dh, N_COL), at(s_ln, N_ROW)
    return pl.pallas_call(
        functools.partial(tail_kernel, n_dev=n_dev),
        grid=(s_ln + N_ROW,),
        in_specs=[pl.BlockSpec((t // K_STEP, chunk), h_map),
                  pl.BlockSpec((dim, cw), lambda s: (0, col_a(s))),
                  pl.BlockSpec((cw, dim), lambda s: (col_h(s), 0)),
                  pl.BlockSpec((cw, kv), lambda s: (col_h(s), 0)),
                  pl.BlockSpec((cw, kv), lambda s: (col_h(s), 0)),
                  pl.BlockSpec((br, dim), lambda s: (row_l(s), 0)),
                  pl.BlockSpec((1, dim), fixed),
                  hbm, hbm, hbm],
        out_specs=[pl.BlockSpec((rows, cw), lambda s: (0, col_a(s))),
                   pl.BlockSpec((br, dim), lambda s: (row_l(s), 0)),
                   pl.BlockSpec((1, dim), fixed),
                   hbm, hbm],
        out_shape=[shape((rows, dim), bf16), shape((rows, dim), bf16),
                   shape((1, dim), bf16), shape((n_dev * dim, width), bf16),
                   shape((n_dev, rows, width - early), bf16)],
        scratch_shapes=[pltpu.VMEM((t, width), bf16), dma, pltpu.VMEM((width, t), bf16), pltpu.VMEM((width, chunk), f32), pltpu.VMEM((2, chunk, width), bf16),
                        pltpu.VMEM((rows, dim + 2 * kv), bf16), pltpu.VMEM((rows, dim), f32), pltpu.VMEM((n_dev, 8, dim), f32),
                        dma((n_dev,)), dma((n_dev,)), dma((7, N_CHUNK)), dma((7, N_CHUNK)),
                        dma((n_dev,)), dma((n_dev,)), dma((2,)), dma((5, n_dev))],
        compiler_params=params(1, collective_id=1),
        name="tail")(h_all, w_o, w_q, w_k, w_v, x, lnw, g_own, g_tok, o_tok)


def spread_kernel(src_ref, a_ref, dx_ref, wo_ref, q_ref, k_ref, v_ref, a_out, dx_out, wo_out):
    n_dev, _, width = src_ref.shape
    qe = width - 2 * D
    for dev in range(n_dev):
        q_ref[:, dev * qe:(dev + 1) * qe] = src_ref[dev, :, :qe]
        k_ref[:, dev * D:(dev + 1) * D] = src_ref[dev, :, qe:qe + D]
        v_ref[:, dev * D:(dev + 1) * D] = src_ref[dev, :, qe + D:]
    a_out[:] = a_ref[:]
    dx_out[:] = dx_ref[:]
    wo_out[:] = wo_ref[:]


def spread(dw_all, a, dx, dwo, steps=12):
    n_dev, dim, width = dw_all.shape
    bt = dim // steps
    qe = width - 2 * D
    same = [(x, pl.BlockSpec((x.shape[0] // steps, x.shape[1]), rows_at)) for x in (a, dx, dwo)]
    cols = [n_dev * c for c in (qe, D, D)]
    return pl.pallas_call(
        spread_kernel,
        grid=(steps,),
        in_specs=[pl.BlockSpec((n_dev, bt, width), lambda i: (0, i, 0))] + [spec for _, spec in same],
        out_specs=[pl.BlockSpec((bt, c), rows_at) for c in cols] + [spec for _, spec in same],
        out_shape=[shape((dim, c), bf16) for c in cols] + [shape(x.shape, bf16) for x, _ in same],
        compiler_params=params(),
        name="spread")(dw_all, a, dx, dwo)


def solution(mesh):
    n_dev = mesh.shape['sp']
    row_spec = P(('dp', 'sp'), None)
    pos_spec = P(('dp', 'sp'))
    full_spec = P(None, None)
    grad_spec = P('dp', None)

    def local_step(hidden, positions, d_attn, ln_weight, w_q, w_k, w_v, w_o):
        rows, dim = hidden.shape
        qe = w_q.shape[1] // n_dev
        ke = w_k.shape[1] // n_dev
        lane = jnp.arange(D, dtype=jnp.int32)
        freq = ROPE_BASE ** (-(lane - lane % 2).astype(f32) / D)
        pos = jnp.pad(positions.reshape(N_SUB, rows // N_SUB // D, D), ((0, 0), (0, 8 - rows // N_SUB // D), (0, 0)))
        q, qt, k, v, vt, cos, sin, h_all = start(hidden, ln_weight.reshape(1, dim), w_q, w_k, w_v, freq.reshape(1, D), pos, qe // D, n_dev)
        o, ot, lse, g_first = attn_fwd(q, k, vt, d_attn, rows * 2 // 3, n_dev)
        do, dot, dwo_own, _ = mid(g_first, ot, w_o, d_attn, n_dev)
        g_own, o_tok, g_tok, dw_o = attn_bwd(q, qt, do, dot, o, lse, k, v, cos, sin, dwo_own, n_dev)
        attn_out, d_hid, d_lnw, dw_all, _ = tail(h_all, g_own, g_tok, o_tok, w_o, w_q, w_k, w_v, hidden,
                                                 ln_weight.reshape(1, dim), n_dev)
        dw_q, dw_k, dw_v, attn_out, d_hid, dw_o = spread(dw_all.reshape(n_dev, dim, qe + 2 * ke), attn_out, d_hid, dw_o)
        return attn_out, d_hid, d_lnw.reshape(dim), dw_q, dw_k, dw_v, dw_o

    return jax.shard_map(local_step, mesh=mesh,
                         in_specs=(row_spec, pos_spec, row_spec, P(None), full_spec, full_spec, full_spec, full_spec),
                         out_specs=(row_spec, row_spec, P('dp'), grad_spec, grad_spec, grad_spec, grad_spec),
                         check_vma=False)
```
